32 devices in a mesh: row: 8 (over y, x, core), col: 4 (over z).
Axes of the slice: x: 2, y: 2, z: 4, core: 2. Of those that a mesh axis runs over, the one named last changes fastest.
Arguments:
- columns: float32 [4096, 8192], P('col', 'row'), may hold values from -64 to 64
- block_order: int32 [64], P('col'), may hold values from 0 to 63, as said below
Outputs:
- rotated: float32 [4096, 8192], P('col', 'row')
The draws below stay inside these ranges and needn't reach their ends.
Inputs may be any that keep to these rules, and one draw needn't show every extreme that they name: block_order is a permutation of 0 .. 63 in which slots c * 16 to (c + 1) * 16 - 1 name blocks c * 16 to (c + 1) * 16 - 1.
All inputs are finite; a program needn't handle non-finite values.
Results may differ from the reference program's by a relative error of at most 0.00055.
Values sent between devices are 32-bit elements; how exact they have to be, the bound alone decides.
No kernel may reach another device: no remote copies, remote signals or barrier semaphores. Data moves between devices by JAX's collectives and lax.ppermute only.
A program may use at most 64 MiB of HBM per device.

```python
import math
import jax
import jax.numpy as jnp
from jax import lax

BLOCK = 64
STEPS = 4
BLOCKS_DEV = 16
N = 4096
M = 8192
BLOCKS = 64


def draw_columns(key, part):
    keys = jax.random.split(key, 4)
    gain_rows = 1.0 + 2.0 * jnp.arange(M, dtype=jnp.float32) / M
    loadings = jax.random.truncated_normal(keys[2], -3.0, 3.0, (N,), jnp.float32)
    noise = jax.random.truncated_normal(keys[0], -4.0, 4.0, (N, M), jnp.float32)
    scales = jnp.exp(jax.random.uniform(keys[1], (N,), jnp.float32, math.log(0.3), math.log(3.0)))
    common = jax.random.truncated_normal(keys[3], -3.0, 3.0, (M,), jnp.float32)
    return noise * scales[:, None] + loadings[:, None] * (common * gain_rows)[None, :]


def draw_block_order(key, part):
    groups = BLOCKS // BLOCKS_DEV
    scores = jax.random.randint(key, (groups, BLOCKS_DEV), 0, 1 << 20) * BLOCKS_DEV + jnp.arange(BLOCKS_DEV, dtype=jnp.int32)[None, :]
    shuffled = jnp.argsort(scores, axis=1, stable=True).astype(jnp.int32)
    return (shuffled + (jnp.arange(groups, dtype=jnp.int32) * BLOCKS_DEV)[:, None]).reshape(-1)


def setup_inputs(seed: int = 0) -> dict:
    splits = jax.random.split(jax.random.key(seed), 3)
    return {
        "columns": draw_columns(jax.random.fold_in(splits[2], 71), 0),
        "block_order": draw_block_order(jax.random.fold_in(splits[2], 71), 0),
    }


def cayley_turn(cross_sum, col_norms):
    highest = lax.Precision.HIGHEST
    top_norms = col_norms[:, :BLOCK][:, :, None]
    bottom_norms = col_norms[:, BLOCK:][:, None, :]
    spread = bottom_norms - top_norms
    radius = jnp.sqrt(spread * spread + 4.0 * cross_sum * cross_sum)
    scale_term = (top_norms + bottom_norms) / BLOCK
    coupling = 2.0 * cross_sum * spread / (spread * spread + 4.0 * cross_sum * cross_sum + jnp.abs(spread) * radius + scale_term * scale_term)
    identity = jnp.eye(BLOCK, dtype=jnp.float32)
    left_system = identity + jnp.einsum('pij,pkj->pik', coupling, coupling, precision=highest)
    right_system = identity + jnp.einsum('pji,pjk->pik', coupling, coupling, precision=highest)
    left_factor = jnp.linalg.cholesky(left_system)
    right_factor = jnp.linalg.cholesky(right_system)
    identities = jnp.broadcast_to(identity, coupling.shape)
    upper_half = jnp.concatenate([identities, coupling], axis=2)
    lower_half = jnp.concatenate([-jnp.transpose(coupling, (0, 2, 1)), identities], axis=2)

    def solve_one(factor, target):
        return jax.scipy.linalg.cho_solve((factor, True), target)
    upper_solved = jax.vmap(solve_one)(left_factor, upper_half)
    lower_solved = jax.vmap(solve_one)(right_factor, lower_half)
    solved = jnp.concatenate([upper_solved, lower_solved], axis=1)
    plus_skew = jnp.concatenate([upper_half, lower_half], axis=1)
    return jnp.einsum('pij,pjk->pik', plus_skew, solved, precision=highest)

def reference(columns, block_order):
    highest = lax.Precision.HIGHEST
    width, length = columns.shape
    count = width // BLOCK
    blocks = jnp.take(columns.reshape(count, BLOCK, length), block_order.astype(jnp.int32), axis=0)
    blocks = blocks.reshape(count // 2, 2 * BLOCK, length)
    for sweep_step in range(STEPS):
        gram_sum = jnp.einsum('pim,pjm->pij', blocks, blocks, precision=highest)
        col_norms = jnp.diagonal(gram_sum, axis1=1, axis2=2)
        cross_sum = gram_sum[:, :BLOCK, BLOCK:]
        turn_matrix = cayley_turn(cross_sum, col_norms)
        turned = jnp.einsum('pij,pim->pjm', turn_matrix, blocks, precision=highest)
        top_blocks = turned[:, :BLOCK]
        bottom_blocks = turned[:, BLOCK:]
        new_tops = jnp.concatenate([top_blocks[:1], bottom_blocks[:1], top_blocks[1:-1]], axis=0)
        new_bottoms = jnp.concatenate([bottom_blocks[1:], top_blocks[-1:]], axis=0)
        blocks = jnp.concatenate([new_tops, new_bottoms], axis=1)
    return blocks.reshape(width, length)
```

```python
import jax
import jax.numpy as jnp
from jax import lax
from jax.experimental import pallas as pl
from jax.experimental.pallas import tpu as pltpu
from jax.sharding import PartitionSpec as P

BLOCK = 64
STEPS = 4
RANK = 8
LANES = 2 * BLOCK
ROWS = 2 * BLOCK + 8


f32 = jnp.float32
bf16 = jnp.bfloat16
SMEM = pl.BlockSpec(memory_space=pltpu.SMEM)
VMEM = pl.BlockSpec(memory_space=pltpu.VMEM)


def split(value):
    high = value.astype(bf16)
    low = (value - high.astype(f32)).astype(bf16)
    return high, low


def lane_index(rows):
    return lax.broadcasted_iota(jnp.int32, (rows, LANES), 1)


def put_split(ref, slot, value):
    high, low = split(value)
    ref[slot, :BLOCK, :] = high
    ref[slot, BLOCK:, :] = low


def cross_twice(top, bottom):
    gram = lax.dot_general(top, bottom, (((1,), (1,)), ((), ())), preferred_element_type=f32)
    folded = gram[:BLOCK] + gram[BLOCK:]
    return folded + pltpu.roll(folded, BLOCK, 1)


def square_sum(value):
    return jnp.sum(value * value, axis=1, keepdims=True)


def put_halves(core, packed_ref, mine_ref, other_ref):
    mine_ref[...] = packed_ref[core]
    other_ref[...] = packed_ref[1 - core]


def start_kernel(order_ref, where_ref, top0, bottom0, top1, bottom1, split_ref, mine_ref, other_ref, packed, norms):
    group = pl.program_id(0)
    lane = lane_index(BLOCK)

    @pl.when(group == 0)
    def _():
        packed[...] = jnp.zeros_like(packed)
        norms[...] = jnp.zeros_like(norms)

    crosses = []
    for index, (top_in, bottom_in) in enumerate(((top0, bottom0), (top1, bottom1))):
        for half, value_ref in enumerate((top_in, bottom_in)):
            value = value_ref[0]
            put_split(split_ref, 2 * index + half, value)
            rows = pl.ds(half * BLOCK, BLOCK)
            norms[rows, :] = jnp.where(lane == 2 * group + index, square_sum(value), norms[rows, :])
        crosses.append(cross_twice(split_ref[2 * index], split_ref[2 * index + 1]))
    rows = pl.ds(pl.multiple_of((group % 2) * BLOCK, BLOCK), BLOCK)
    packed[group // 2, rows, :] = jnp.where(lane < BLOCK, crosses[0], crosses[1])

    @pl.when(group == pl.num_programs(0) - 1)
    def _():
        by_pair = norms[...].T
        packed[0, 2 * BLOCK : 2 * BLOCK + 4, :] = by_pair[0:4]
        packed[1, 2 * BLOCK : 2 * BLOCK + 4, :] = by_pair[4:8]
        put_halves(where_ref[0], packed, mine_ref, other_ref)


def start(columns, order, where):
    count, _, length = columns.shape

    def block_at(slot):
        return pl.BlockSpec((1, BLOCK, length), lambda g, order_ref, where_ref: (order_ref[4 * g + slot], 0, 0))

    half = jax.ShapeDtypeStruct((ROWS, LANES), f32)
    return pl.pallas_call(
        start_kernel,
        grid_spec=pltpu.PrefetchScalarGridSpec(
            num_scalar_prefetch=2,
            grid=(count // 4,),
            in_specs=[block_at(slot) for slot in range(4)],
            out_specs=[
                pl.BlockSpec((4, LANES, length), lambda g, *_: (g, 0, 0)),
                pl.BlockSpec((ROWS, LANES), lambda g, *_: (0, 0)),
                pl.BlockSpec((ROWS, LANES), lambda g, *_: (0, 0)),
            ],
            scratch_shapes=[pltpu.VMEM((2, ROWS, LANES), f32), pltpu.VMEM((LANES, LANES), f32)],
        ),
        out_shape=[jax.ShapeDtypeStruct((count, LANES, length), bf16), half, half],
        compiler_params=pltpu.CompilerParams(vmem_limit_bytes=12 << 20),
        name="start",
    )(order, where, columns, columns, columns, columns)


def row_of(value, index):
    return jnp.broadcast_to(value[index : index + 1, :], value.shape)


def eliminate(blocks, panels):
    size = len(blocks[0])
    sublane = lax.broadcasted_iota(jnp.int32, (size, LANES), 0)
    for j in range(size):
        here = sublane == j
        for q, work in enumerate(blocks):
            pivot_column = work[j]
            inverse = 1.0 / row_of(pivot_column, j)

            def swept(value):
                scaled = row_of(value, j) * inverse
                return jnp.where(here, scaled, value - pivot_column * scaled)

            for b in range(j + 1, size):
                work[b] = swept(work[b])
            panels[q] = swept(panels[q])
    return panels


def inverses(systems):
    lane = lane_index(RANK)
    base = (lane // BLOCK) * BLOCK
    eye = (lax.broadcasted_iota(jnp.int32, (RANK, LANES), 0) == lane % RANK).astype(f32)
    groups = BLOCK // RANK
    work = [[system[RANK * g : RANK * (g + 1)] for g in range(groups)] for system in systems]
    for r in range(groups):
        pivots = (lane % BLOCK) // RANK == r
        order = [(r + i) % groups for i in range(groups)]
        columns = [[[None] * RANK for _ in range(groups)] for _ in work]
        for some in (order[:1], order[1:]):
            for a in range(RANK):
                pick = base + (RANK * r + a)
                for g in some:
                    for q, rows in enumerate(work):
                        columns[q][g][a] = jnp.take_along_axis(rows[g], pick, axis=1, mode="promise_in_bounds")
        panels = eliminate(
            [list(columns[q][r]) for q in range(len(work))], [jnp.where(pivots, eye, rows[r]) for rows in work]
        )
        updates = []
        for q, rows in enumerate(work):
            rows[r] = jnp.where(pivots, -panels[q], panels[q])
            used = jnp.where(pivots, eye - panels[q], panels[q])
            updates.append([row_of(used, a) for a in range(RANK)])
        for g in order[1:]:
            for q, rows in enumerate(work):
                value = rows[g]
                for a in range(RANK):
                    value = value - columns[q][g][a] * updates[q][a]
                rows[g] = value
    return [-jnp.concatenate(rows, axis=0) for rows in work]


def split3(value):
    high = value.astype(bf16)
    rest = value - high.astype(f32)
    middle = rest.astype(bf16)
    return high, middle, (rest - middle.astype(f32)).astype(bf16)


def product3(left, right, transposed=False):
    axis = 1 if transposed else 0
    contract = (((1,), (axis,)), ((), ()))

    def dot(lefts, rights):
        return lax.dot_general(
            jnp.concatenate(lefts, axis=1), jnp.concatenate(rights, axis=axis), contract, preferred_element_type=f32
        )

    high, middle, low = left
    other_high, other_middle, other_low = right
    return (
        dot((low, high), (other_high, other_low))
        + dot((high, middle), (other_middle, other_middle))
        + dot((high, middle), (other_high, other_high))
    )


def apply_turn(full, rest, top, bottom):
    both = jnp.concatenate([top, bottom], axis=0)
    highs = jnp.concatenate([top[:BLOCK], bottom[:BLOCK]] * 2, axis=0)
    return jnp.dot(full, both, preferred_element_type=f32) + jnp.dot(rest, highs, preferred_element_type=f32)


def turn_kernel(where_ref, mine_ref, other_ref, first_top, first_bottom, last_top, last_bottom, full_ref, rest_ref, even_ref, odd_ref):
    pairs = full_ref.shape[0]
    each = range(pairs // 2)
    core = where_ref[0]
    lane = lane_index(BLOCK)
    left = lane < BLOCK
    unit = (lax.broadcasted_iota(jnp.int32, (BLOCK, LANES), 0) == lane % BLOCK).astype(f32)

    def diagonal(value):
        zero = jnp.zeros_like(value)
        return jnp.concatenate([jnp.where(left, value, zero), jnp.where(left, zero, value)], axis=0)

    def turn_over(value):
        return pltpu.roll(value, BLOCK, 1)

    mine, other = mine_ref[...], other_ref[...]
    halves = [jnp.where(core == 0, mine, other), jnp.where(core == 0, other, mine)]
    norm_rows = jnp.concatenate([half[2 * BLOCK : 2 * BLOCK + 4] for half in halves], axis=0)
    by_column = jnp.concatenate([norm_rows, jnp.zeros((LANES - pairs, LANES), f32)], axis=0).T
    flipped = turn_over(norm_rows)
    couplings = []
    for q in each:
        cross = halves[q // 2][(q % 2) * BLOCK : (q % 2 + 1) * BLOCK]
        p0, p1 = 2 * q, 2 * q + 1
        bottom = jnp.where(left[:1], flipped[p0 : p0 + 1], norm_rows[p1 : p1 + 1])
        top = jnp.where(left, by_column[:BLOCK, p0 : p0 + 1], by_column[:BLOCK, p1 : p1 + 1])
        spread = bottom - top
        square = spread * spread + 4.0 * cross * cross
        scale = (top + bottom) / BLOCK
        couplings.append(2.0 * cross * spread / (square + jnp.abs(spread) * jnp.sqrt(square) + scale * scale))
    parts = [split3(coupling) for coupling in couplings]
    spread_parts = [tuple(diagonal(part) for part in parts[q]) for q in each]
    systems = [unit + product3(parts[q], spread_parts[q], True) for q in each]
    flips = [split3(jnp.concatenate([coupling, coupling], axis=0).T) for coupling in couplings]

    solved = inverses(systems)

    products = [product3(split3(solved[q]), spread_parts[q]) for q in each]
    residuals = [unit - solved[q] - product3(split3(products[q]), spread_parts[q], True) for q in each]
    steps = [
        jnp.dot(residuals[q].astype(bf16), diagonal(solved[q].astype(bf16)), preferred_element_type=f32) for q in each
    ]
    solved = [solved[q] + steps[q] for q in each]
    products = [
        products[q] + jnp.dot(steps[q].astype(bf16), spread_parts[q][0], preferred_element_type=f32) for q in each
    ]
    corners = []
    for q in each:
        high, middle, low = split3(products[q])
        flip_high, flip_middle, flip_low = flips[q]
        mixed = jnp.where(lane_index(LANES) < BLOCK, flip_low, flip_high)
        corners.append(
            jnp.dot(mixed, jnp.concatenate([high, low], axis=0), preferred_element_type=f32)
            + jnp.dot(
                jnp.concatenate([flip_high, flip_middle], axis=1),
                jnp.concatenate([high, middle, high, middle], axis=0),
                preferred_element_type=f32,
            )
        )
    products_t = [jnp.concatenate([product, product], axis=0).T for product in products]

    def put(pair, rows, top_part, bottom_part):
        full_ref[pair, rows, :LANES] = top_part.astype(bf16)
        full_ref[pair, rows, LANES:] = bottom_part.astype(bf16)
        _, middle, low = split3(jnp.where(left, top_part, bottom_part))
        rest_ref[pair, rows, :LANES] = middle
        rest_ref[pair, rows, LANES:] = low

    upper_rows, lower_rows = slice(0, BLOCK), slice(BLOCK, LANES)
    for q in each:
        pair = 2 * q
        inverse, product, corner = solved[q], products[q], corners[q]
        inverse_r, product_r = turn_over(inverse), turn_over(product)
        first_corner, second_corner = corner[:BLOCK], corner[BLOCK:]
        first_r, second_r = turn_over(first_corner), turn_over(second_corner)
        doubles = (
            (jnp.where(left, inverse, inverse_r), jnp.where(left, product, product_r), products_t[q][:BLOCK], jnp.where(left, first_corner, first_r)),
            (jnp.where(left, inverse_r, inverse), jnp.where(left, product_r, product), products_t[q][BLOCK:], jnp.where(left, second_r, second_corner)),
        )
        for h, (inverse2, product2, product_t2, corner2) in enumerate(doubles):
            put(pair + h, upper_rows, 2.0 * inverse2 - unit, -2.0 * product2)
            put(pair + h, lower_rows, 2.0 * product_t2, unit - 2.0 * corner2)

    last = pairs - 1
    last_out = apply_turn(full_ref[last, :BLOCK, :], rest_ref[last, :BLOCK, :], last_top[0], last_bottom[0])
    first_out = apply_turn(full_ref[0, BLOCK:, :], rest_ref[0, BLOCK:, :], first_top[0], first_bottom[0])
    even = where_ref[1] == 0
    even_ref[...] = jnp.where(even, last_out, first_out)
    odd_ref[...] = jnp.where(even, first_out, last_out)


def block_of(array, slot):
    return pl.BlockSpec((1,) + array.shape[1:], lambda *_: (slot, 0, 0))


def turns(where, mine, other, blocks, edges):
    count, _, length = blocks.shape
    pairs = count // 2
    first, last = edges
    split_turn = jax.ShapeDtypeStruct((pairs, LANES, 2 * LANES), bf16)
    sent = jax.ShapeDtypeStruct((BLOCK, length), f32)
    return pl.pallas_call(
        turn_kernel,
        grid=(1,),
        in_specs=[SMEM, VMEM, VMEM, block_of(*first), block_of(blocks, 1), block_of(blocks, count - 2), block_of(*last)],
        out_specs=[VMEM, VMEM, VMEM, VMEM],
        out_shape=[split_turn, split_turn, sent, sent],
        cost_estimate=pl.CostEstimate(flops=10**7, bytes_accessed=10**6, transcendentals=0),
        compiler_params=pltpu.CompilerParams(vmem_limit_bytes=14 << 20),
        name="turns",
    )(where, mine, other, first[0], blocks, blocks, last[0])


def turned_pairs(where_ref, full_ref, rest_ref, blocks_ref, first_ref, last_ref, place):
    pairs = full_ref.shape[0]
    for p in range(pairs):
        top = first_ref[0] if p == 0 else blocks_ref[2 * p]
        bottom = last_ref[0] if p == pairs - 1 else blocks_ref[2 * p + 1]
        out = apply_turn(full_ref[p], rest_ref[p], top, bottom)
        place(p, out[:BLOCK], out[BLOCK:])


def move_kernel(where_ref, full_ref, rest_ref, blocks_ref, first_ref, last_ref, moved_ref, packed_ref):
    pairs = full_ref.shape[0]
    last = pairs - 1
    is_first, is_last = where_ref[2] == 1, where_ref[3] == 1
    lane = lane_index(BLOCK)
    norms = [jnp.zeros((BLOCK, LANES), f32), jnp.zeros((BLOCK, LANES), f32)]
    kept = {}

    def place(p, top, bottom):
        top_sum, bottom_sum = square_sum(top), square_sum(bottom)
        if p == 0:
            put_split(moved_ref, 0, top)
            put_split(moved_ref, 2, jnp.where(is_first, bottom, top))
            norms[0] = jnp.where(lane == 0, top_sum, norms[0])
            norms[0] = jnp.where(lane == 1, jnp.where(is_first, bottom_sum, top_sum), norms[0])
        else:
            put_split(moved_ref, 2 * p - 1, bottom)
            norms[1] = jnp.where(lane == p - 1, bottom_sum, norms[1])
            if p == last:
                put_split(moved_ref, 2 * p + 1, top)
                norms[1] = jnp.where(lane == p, top_sum, norms[1])
            else:
                put_split(moved_ref, 2 * p + 2, top)
                norms[0] = jnp.where(lane == p + 1, top_sum, norms[0])

    turned_pairs(where_ref, full_ref, rest_ref, blocks_ref, first_ref, last_ref, place)
    for p in range(1, last):
        kept[p] = cross_twice(moved_ref[2 * p], moved_ref[2 * p + 1])
    kept[0] = kept[last] = jnp.zeros((BLOCK, LANES), f32)
    by_pair = jnp.concatenate(norms, axis=0).T
    for q in range(pairs // 2):
        rows = slice((q % 2) * BLOCK, (q % 2 + 1) * BLOCK)
        packed_ref[q // 2, rows, :] = jnp.where(lane < BLOCK, kept[2 * q], kept[2 * q + 1])
    for half in range(2):
        packed_ref[half, 2 * BLOCK : 2 * BLOCK + 4, :] = by_pair[4 * half : 4 * half + 4]
        packed_ref[half, 2 * BLOCK + 4 :, :] = jnp.zeros((4, LANES), f32)


def final_kernel(where_ref, full_ref, rest_ref, blocks_ref, first_ref, last_ref, out_ref):
    pairs = full_ref.shape[0]
    last = pairs - 1
    is_first = where_ref[2] == 1

    def place(p, top, bottom):
        if p == 0:
            out_ref[0] = top
            out_ref[2] = jnp.where(is_first, bottom, top)
        else:
            out_ref[2 * p - 1] = bottom
            out_ref[2 * p + 1 if p == last else 2 * p + 2] = top

    turned_pairs(where_ref, full_ref, rest_ref, blocks_ref, first_ref, last_ref, place)


def move(where, full, rest, blocks, edges, final):
    count, _, length = blocks.shape
    first, last = edges
    if final:
        out_shape = jax.ShapeDtypeStruct((count, BLOCK, length), f32)
    else:
        out_shape = [
            jax.ShapeDtypeStruct(blocks.shape, bf16),
            jax.ShapeDtypeStruct((2, ROWS, LANES), f32),
        ]
    return pl.pallas_call(
        final_kernel if final else move_kernel,
        grid=(1,),
        in_specs=[SMEM, VMEM, VMEM, VMEM, block_of(*first), block_of(*last)],
        out_specs=VMEM if final else [VMEM, VMEM],
        out_shape=out_shape,
        cost_estimate=pl.CostEstimate(flops=2 * 10**9, bytes_accessed=10**7, transcendentals=0),
        compiler_params=pltpu.CompilerParams(vmem_limit_bytes=24 << 20),
        name="final" if final else "move",
    )(where, full, rest, blocks, first[0], last[0])


def edge_kernel(where_ref, packed_ref, even_ref, odd_ref, top0, bottom0, top1, bottom1, edge_ref, mine_ref, other_ref, packed):
    even, is_first, is_last = where_ref[1] == 0, where_ref[2] == 1, where_ref[3] == 1
    lane = lane_index(BLOCK)

    def whole(ref):
        return ref[0, :BLOCK, :].astype(f32) + ref[0, BLOCK:, :].astype(f32)

    from_even, from_odd = even_ref[...], odd_ref[...]
    new_top = jnp.where(is_first, whole(top0), jnp.where(even, from_odd, from_even))
    new_bottom = jnp.where(is_last, whole(bottom1), jnp.where(even, from_even, from_odd))
    put_split(edge_ref, 0, new_top)
    put_split(edge_ref, 1, new_bottom)
    packed[...] = packed_ref[...]
    low = cross_twice(edge_ref[0], bottom0[0])
    high = cross_twice(top1[0], edge_ref[1])
    packed[0, :BLOCK, :] = jnp.where(lane < BLOCK, low, packed[0, :BLOCK, :])
    packed[1, BLOCK : 2 * BLOCK, :] = jnp.where(lane < BLOCK, packed[1, BLOCK : 2 * BLOCK, :], high)
    norms = jnp.where(lane == 0, square_sum(new_top), 0.0)
    norms = jnp.concatenate([norms, jnp.where(lane == 1, square_sum(new_bottom), 0.0)], axis=0).T
    row = 2 * BLOCK
    packed[0, row : row + 1, :] = jnp.where(lane[:1] < BLOCK, norms[0:1], packed[0, row : row + 1, :])
    packed[1, row + 3 : row + 4, :] = jnp.where(lane[:1] < BLOCK, packed[1, row + 3 : row + 4, :], norms[1:2])
    put_halves(where_ref[0], packed, mine_ref, other_ref)


def join(where, packed, even, odd, moved):
    count, _, length = moved.shape
    half = jax.ShapeDtypeStruct((ROWS, LANES), f32)
    return pl.pallas_call(
        edge_kernel,
        grid=(1,),
        in_specs=[SMEM, VMEM, VMEM, VMEM] + [block_of(moved, slot) for slot in (0, 1, count - 2, count - 1)],
        out_specs=[VMEM, VMEM, VMEM],
        out_shape=[jax.ShapeDtypeStruct((2, LANES, length), bf16), half, half],
        scratch_shapes=[pltpu.VMEM((2, ROWS, LANES), f32)],
        cost_estimate=pl.CostEstimate(flops=10**7, bytes_accessed=10**6, transcendentals=0),
        compiler_params=pltpu.CompilerParams(vmem_limit_bytes=8 << 20),
        name="join",
    )(where, packed, even, odd, moved, moved, moved, moved)


def last_kernel(where_ref, even_ref, odd_ref, own_ref, out_ref):
    even, edge = where_ref[1] == 0, pl.program_id(0)
    own = jnp.where(edge == 0, where_ref[2], where_ref[3]) == 1
    use_odd = even == (edge == 0)
    out_ref[0] = jnp.where(own, own_ref[0], jnp.where(use_odd, odd_ref[...], even_ref[...]))


def close(where, even, odd, out):
    count = out.shape[0]
    spec = pl.BlockSpec((1,) + out.shape[1:], lambda g: (g * (count - 1), 0, 0))
    return pl.pallas_call(
        last_kernel,
        grid=(2,),
        in_specs=[SMEM, VMEM, VMEM, spec],
        out_specs=spec,
        out_shape=jax.ShapeDtypeStruct(out.shape, f32),
        input_output_aliases={3: 0},
        compiler_params=pltpu.CompilerParams(vmem_limit_bytes=8 << 20),
        name="close",
    )(where, even, odd, out)


def exchange(value, bit):
    count = lax.axis_size("row")
    return lax.ppermute(value, "row", [(source, source ^ bit) for source in range(count)])


def row_sum(mine, other):
    count = lax.axis_size("row")
    total = mine + exchange(other, 1)
    if count == 8:
        near, far, across = exchange(total, 2), exchange(total, 4), exchange(total, 6)
        total = (total + near) + (far + across)
    else:
        bit = 2
        while bit < count:
            total = total + exchange(total, bit)
            bit *= 2
    return total, exchange(total, 1)


def swap_edges(even, odd):
    count = lax.axis_size("col")

    def between(start):
        pairs = [(left, left + 1) for left in range(start, count - 1, 2)]
        return pairs + [(right, left) for left, right in pairs]

    return lax.ppermute(even, "col", between(0)), lax.ppermute(odd, "col", between(1))


def local(columns, block_order):
    width, length = columns.shape
    count = width // BLOCK
    assert count == 16 and lax.axis_size("row") % 2 == 0
    position = lax.axis_index("col")
    where = jnp.stack(
        [
            lax.axis_index("row") % 2,
            position % 2,
            (position == 0).astype(jnp.int32),
            (position == lax.axis_size("col") - 1).astype(jnp.int32),
        ]
    ).astype(jnp.int32)
    order = block_order - position * count
    blocks, mine, other = start(columns.reshape(count, BLOCK, length), order, where)
    edges = ((blocks, 0), (blocks, count - 1))
    for step in range(STEPS):
        final = step == STEPS - 1
        mine, other = row_sum(mine, other)
        full, rest, even, odd = turns(where, mine, other, blocks, edges)
        even, odd = swap_edges(even, odd)
        if final:
            out = move(where, full, rest, blocks, edges, True)
            return close(where, even, odd, out).reshape(width, length)
        blocks, packed = move(where, full, rest, blocks, edges, False)
        edge, mine, other = join(where, packed, even, odd, blocks)
        edges = ((edge, 0), (edge, 1))


def solution(mesh):
    placed = (P("col", "row"), P("col"))
    return jax.shard_map(local, mesh=mesh, in_specs=placed, out_specs=P("col", "row"), check_vma=False)
```

```python
import jax
import jax.numpy as jnp
from jax import lax
from jax.experimental import pallas as pl
from jax.experimental.pallas import tpu as pltpu
from jax.sharding import PartitionSpec as P

BLOCK = 64
STEPS = 4
RANK = 8
LANES = 2 * BLOCK
AHEAD = 4
ROWS = 2 * BLOCK + 8


f32 = jnp.float32
bf16 = jnp.bfloat16
SMEM = pl.BlockSpec(memory_space=pltpu.SMEM)
VMEM = pl.BlockSpec(memory_space=pltpu.VMEM)


def split(value):
    high = value.astype(bf16)
    low = (value - high.astype(f32)).astype(bf16)
    return high, low


def lane_index(rows):
    return lax.broadcasted_iota(jnp.int32, (rows, LANES), 1)


def put_split(ref, slot, value):
    high, low = split(value)
    ref[slot, :BLOCK, :] = high
    ref[slot, BLOCK:, :] = low


def cross_twice(top, bottom):
    gram = lax.dot_general(top, bottom, (((1,), (1,)), ((), ())), preferred_element_type=f32)
    folded = gram[:BLOCK] + gram[BLOCK:]
    return folded + pltpu.roll(folded, BLOCK, 1)


def square_sum(value):
    return jnp.sum(value * value, axis=1, keepdims=True)


def flag(flags_ref, row, lanes=LANES):
    return flags_ref[row : row + 1, :lanes] == 1


def put_halves(flags_ref, packed_ref, mine_ref, other_ref):
    core = flag(flags_ref, 0)
    mine_ref[...] = jnp.where(core, packed_ref[1], packed_ref[0])
    other_ref[...] = jnp.where(core, packed_ref[0], packed_ref[1])


def place_of(pair, pairs):
    return 0 if pair == 0 else 1 if pair == pairs - 1 else pair + 1


def put_norms(packed_ref, by_place):
    for half in range(2):
        packed_ref[half, 2 * BLOCK : 2 * BLOCK + 4, :] = by_place[4 * half : 4 * half + 4]
        packed_ref[half, 2 * BLOCK + 4 :, :] = jnp.zeros((4, LANES), f32)


def start_kernel(order_ref, flags_ref, columns_ref, split_ref, mine_ref, other_ref, held, packed, sems):
    count = held.shape[0]
    pairs = count // 2
    lane = lane_index(BLOCK)

    def fetch(slot):
        return pltpu.make_async_copy(columns_ref.at[order_ref[slot]], held.at[slot], sems.at[slot])

    by_position = [0, pairs - 1] + list(range(1, pairs - 1))

    def ask(position):
        if position < pairs:
            fetch(2 * by_position[position]).start()
            fetch(2 * by_position[position] + 1).start()

    for position in range(AHEAD):
        ask(position)
    sums = [jnp.zeros((BLOCK, LANES), f32), jnp.zeros((BLOCK, LANES), f32)]
    crosses = []
    for position in range(pairs):
        pair = by_position[position]
        fetch(2 * pair).wait()
        fetch(2 * pair + 1).wait()
        ask(position + AHEAD)
        for half in range(2):
            slot = 2 * pair + half
            value = held[slot]
            put_split(split_ref, slot, value)
            sums[half] = jnp.where(lane == position, square_sum(value), sums[half])
        crosses.append(cross_twice(split_ref[2 * pair], split_ref[2 * pair + 1]))
    for q in range(pairs // 2):
        rows = slice((q % 2) * BLOCK, (q % 2 + 1) * BLOCK)
        packed[q // 2, rows, :] = jnp.where(lane < BLOCK, crosses[2 * q], crosses[2 * q + 1])
    put_norms(packed, jnp.concatenate(sums, axis=0).T)
    put_halves(flags_ref, packed, mine_ref, other_ref)


def start(columns, order, flags):
    count, _, length = columns.shape
    half = jax.ShapeDtypeStruct((ROWS, LANES), f32)
    return pl.pallas_call(
        start_kernel,
        in_specs=[SMEM, VMEM, pl.BlockSpec(memory_space=pltpu.HBM)],
        out_specs=[VMEM, VMEM, VMEM],
        out_shape=[jax.ShapeDtypeStruct((count, LANES, length), bf16), half, half],
        scratch_shapes=[
            pltpu.VMEM((count, BLOCK, length), f32),
            pltpu.VMEM((2, ROWS, LANES), f32),
            pltpu.SemaphoreType.DMA((count,)),
        ],
        compiler_params=pltpu.CompilerParams(vmem_limit_bytes=46 << 20),
        name="start",
    )(order, flags, columns)


def row_of(value, index):
    return jnp.broadcast_to(value[index : index + 1, :], value.shape)


def eliminate(blocks, panels):
    size = len(blocks[0])
    sublane = lax.broadcasted_iota(jnp.int32, (size, LANES), 0)
    for j in range(size):
        here = sublane == j
        for q, work in enumerate(blocks):
            pivot_column = work[j]
            factor = jnp.where(here, pivot_column - 1.0, pivot_column) * (1.0 / row_of(pivot_column, j))

            def swept(value):
                return value - factor * row_of(value, j)

            for b in range(j + 1, size):
                work[b] = swept(work[b])
            panels[q] = swept(panels[q])
    return panels


def inverses(systems):
    lane = lane_index(RANK)
    base = (lane // BLOCK) * BLOCK
    eye = (lax.broadcasted_iota(jnp.int32, (RANK, LANES), 0) == lane % RANK).astype(f32)
    groups = BLOCK // RANK

    def sweep(r, work):
        pivots = (lane % BLOCK) // RANK == r
        columns = [[[None] * RANK for _ in range(groups)] for _ in work]
        for some in (range(1), range(1, groups)):
            for a in range(RANK):
                pick = base + (RANK * r + a)
                for g in some:
                    for q, rows in enumerate(work):
                        columns[q][g][a] = jnp.take_along_axis(rows[g], pick, axis=1, mode="promise_in_bounds")
        panels = eliminate(
            [list(columns[q][0]) for q in range(len(work))], [jnp.where(pivots, eye, rows[0]) for rows in work]
        )
        result = []
        for q, rows in enumerate(work):
            used = jnp.where(pivots, eye - panels[q], panels[q])
            update = [row_of(used, a) for a in range(RANK)]
            swept = []
            for g in range(1, groups):
                value = rows[g]
                for a in range(RANK):
                    value = value - columns[q][g][a] * update[a]
                swept.append(value)
            result.append(tuple(swept) + (jnp.where(pivots, -panels[q], panels[q]),))
        return tuple(result)

    work = tuple(tuple(system[RANK * g : RANK * (g + 1)] for g in range(groups)) for system in systems)
    work = lax.fori_loop(0, groups, sweep, work)
    return [-jnp.concatenate(rows, axis=0) for rows in work]


def split3(value):
    high = value.astype(bf16)
    rest = value - high.astype(f32)
    middle = rest.astype(bf16)
    return high, middle, (rest - middle.astype(f32)).astype(bf16)


def product3(left, right, transposed=False):
    axis = 1 if transposed else 0
    contract = (((1,), (axis,)), ((), ()))

    def dot(lefts, rights):
        return lax.dot_general(
            jnp.concatenate(lefts, axis=1), jnp.concatenate(rights, axis=axis), contract, preferred_element_type=f32
        )

    high, middle, low = left
    other_high, other_middle, other_low = right
    return (
        dot((low, high), (other_high, other_low))
        + dot((high, middle), (other_middle, other_middle))
        + dot((high, middle), (other_high, other_high))
    )


def apply_turn(full, rest, top, bottom):
    both = jnp.concatenate([top, bottom], axis=0)
    highs = jnp.concatenate([top[:BLOCK], bottom[:BLOCK]] * 2, axis=0)
    return jnp.dot(full, both, preferred_element_type=f32) + jnp.dot(rest, highs, preferred_element_type=f32)


def couple(flags_ref, mine_ref, other_ref, some, left):
    core = flag(flags_ref, 0)
    mine, other = mine_ref[...], other_ref[...]
    halves = [jnp.where(core, other, mine), jnp.where(core, mine, other)]
    norm_rows = jnp.concatenate([half[2 * BLOCK : 2 * BLOCK + 4] for half in halves], axis=0)
    by_column = norm_rows.T
    flipped = pltpu.roll(norm_rows, BLOCK, 1)
    couplings = []
    for q in some:
        cross = halves[q // 2][(q % 2) * BLOCK : (q % 2 + 1) * BLOCK]
        n0, n1 = 2 * q, 2 * q + 1
        bottom = jnp.where(left[:1], flipped[n0 : n0 + 1], norm_rows[n1 : n1 + 1])
        top = jnp.where(left, by_column[:BLOCK, n0 : n0 + 1], by_column[:BLOCK, n1 : n1 + 1])
        spread = bottom - top
        square = spread * spread + 4.0 * cross * cross
        scale = (top + bottom) / BLOCK
        couplings.append(2.0 * cross * spread / (square + jnp.abs(spread) * jnp.sqrt(square) + scale * scale))
    return couplings


def put_turns(couplings, full_ref, rest_ref):
    each = range(len(couplings))
    lane = lane_index(BLOCK)
    left = lane < BLOCK
    unit = (lax.broadcasted_iota(jnp.int32, (BLOCK, LANES), 0) == lane % BLOCK).astype(f32)

    def diagonal(value):
        zero = jnp.zeros_like(value)
        return jnp.concatenate([jnp.where(left, value, zero), jnp.where(left, zero, value)], axis=0)

    def turn_over(value):
        return pltpu.roll(value, BLOCK, 1)

    parts = [split3(coupling) for coupling in couplings]
    spread_parts = [tuple(diagonal(part) for part in parts[q]) for q in each]
    systems = [unit + product3(parts[q], spread_parts[q], True) for q in each]
    flips = [split3(jnp.concatenate([coupling, coupling], axis=0).T) for coupling in couplings]

    solved = inverses(systems)

    products = [product3(split3(solved[q]), spread_parts[q]) for q in each]
    residuals = [unit - solved[q] - product3(split3(products[q]), spread_parts[q], True) for q in each]
    steps = [
        jnp.dot(residuals[q].astype(bf16), diagonal(solved[q].astype(bf16)), preferred_element_type=f32) for q in each
    ]
    solved = [solved[q] + steps[q] for q in each]
    products = [
        products[q] + jnp.dot(steps[q].astype(bf16), spread_parts[q][0], preferred_element_type=f32) for q in each
    ]
    corners = []
    for q in each:
        high, middle, low = split3(products[q])
        flip_high, flip_middle, flip_low = flips[q]
        mixed = jnp.where(lane_index(LANES) < BLOCK, flip_low, flip_high)
        corners.append(
            jnp.dot(mixed, jnp.concatenate([high, low], axis=0), preferred_element_type=f32)
            + jnp.dot(
                jnp.concatenate([flip_high, flip_middle], axis=1),
                jnp.concatenate([high, middle, high, middle], axis=0),
                preferred_element_type=f32,
            )
        )
    products_t = [jnp.concatenate([product, product], axis=0).T for product in products]

    def put(pair, rows, top_part, bottom_part):
        full_ref[pair, rows, :LANES] = top_part.astype(bf16)
        full_ref[pair, rows, LANES:] = bottom_part.astype(bf16)
        _, middle, low = split3(jnp.where(left, top_part, bottom_part))
        rest_ref[pair, rows, :LANES] = middle
        rest_ref[pair, rows, LANES:] = low

    upper_rows, lower_rows = slice(0, BLOCK), slice(BLOCK, LANES)
    for q in each:
        pair = 2 * q
        inverse, product, corner = solved[q], products[q], corners[q]
        inverse_r, product_r = turn_over(inverse), turn_over(product)
        first_corner, second_corner = corner[:BLOCK], corner[BLOCK:]
        first_r, second_r = turn_over(first_corner), turn_over(second_corner)
        doubles = (
            (jnp.where(left, inverse, inverse_r), jnp.where(left, product, product_r), products_t[q][:BLOCK], jnp.where(left, first_corner, first_r)),
            (jnp.where(left, inverse_r, inverse), jnp.where(left, product_r, product), products_t[q][BLOCK:], jnp.where(left, second_r, second_corner)),
        )
        for h, (inverse2, product2, product_t2, corner2) in enumerate(doubles):
            put(pair + h, upper_rows, 2.0 * inverse2 - unit, -2.0 * product2)
            put(pair + h, lower_rows, 2.0 * product_t2, unit - 2.0 * corner2)


def outer_kernel(flags_ref, mine_ref, other_ref, first_top, first_bottom, last_top, last_bottom, full_ref, rest_ref, even_ref, odd_ref):
    put_turns(couple(flags_ref, mine_ref, other_ref, (0,), lane_index(BLOCK) < BLOCK), full_ref, rest_ref)
    last_out = apply_turn(full_ref[1, :BLOCK, :], rest_ref[1, :BLOCK, :], last_top[0], last_bottom[0])
    first_out = apply_turn(full_ref[0, BLOCK:, :], rest_ref[0, BLOCK:, :], first_top[0], first_bottom[0])
    odd = flag(flags_ref, 1, last_out.shape[1])
    even_ref[...] = jnp.where(odd, first_out, last_out)
    odd_ref[...] = jnp.where(odd, last_out, first_out)


def inner_kernel(flags_ref, mine_ref, other_ref, after_ref, full_ref, rest_ref):
    del after_ref
    some = range(1, full_ref.shape[0] // 2 + 1)
    put_turns(couple(flags_ref, mine_ref, other_ref, some, lane_index(BLOCK) < BLOCK), full_ref, rest_ref)


def block_of(array, slot):
    return pl.BlockSpec((1,) + array.shape[1:], lambda *_: (slot, 0, 0))


def turn_shapes(pairs):
    return [jax.ShapeDtypeStruct((pairs, LANES, 2 * LANES), bf16)] * 2


def outer_turns(flags, mine, other, blocks, edges):
    count, _, length = blocks.shape
    first, last = edges
    sent = jax.ShapeDtypeStruct((BLOCK, length), f32)
    return pl.pallas_call(
        outer_kernel,
        grid=(1,),
        in_specs=[VMEM, VMEM, VMEM, block_of(*first), block_of(blocks, 1), block_of(blocks, count - 2), block_of(*last)],
        out_specs=[VMEM] * 4,
        out_shape=turn_shapes(2) + [sent, sent],
        compiler_params=pltpu.CompilerParams(vmem_limit_bytes=12 << 20),
        cost_estimate=pl.CostEstimate(flops=10**7, bytes_accessed=10**6, transcendentals=0),
        name="outer",
    )(flags, mine, other, first[0], blocks, blocks, last[0])


def inner_turns(flags, mine, other, after, pairs):
    return pl.pallas_call(
        inner_kernel,
        in_specs=[VMEM, VMEM, VMEM, pl.BlockSpec(memory_space=pl.ANY)],
        out_specs=[VMEM] * 2,
        out_shape=turn_shapes(pairs - 2),
        compiler_params=pltpu.CompilerParams(vmem_limit_bytes=12 << 20),
        cost_estimate=pl.CostEstimate(flops=10**10, bytes_accessed=10**6, transcendentals=0),
        name="inner",
    )(flags, mine, other, after)


def turned_pairs(outer_refs, inner_refs, blocks_ref, first_ref, last_ref, place):
    pairs = blocks_ref.shape[0] // 2
    for p in range(pairs):
        top = first_ref[0] if p == 0 else blocks_ref[2 * p]
        bottom = last_ref[0] if p == pairs - 1 else blocks_ref[2 * p + 1]
        if p in (0, pairs - 1):
            full, rest = (ref[min(p, 1)] for ref in outer_refs)
        else:
            full, rest = (ref[p - 1] for ref in inner_refs)
        out = apply_turn(full, rest, top, bottom)
        place(p, out[:BLOCK], out[BLOCK:])


def move_kernel(flags_ref, full0, rest0, full1, rest1, blocks_ref, first_ref, last_ref, moved_ref, packed_ref):
    pairs = blocks_ref.shape[0] // 2
    last = pairs - 1
    is_first = flag(flags_ref, 2, blocks_ref.shape[2])
    lane = lane_index(BLOCK)
    norms = [jnp.zeros((BLOCK, LANES), f32), jnp.zeros((BLOCK, LANES), f32)]
    kept = {}

    def mark(part, pair, value):
        norms[part] = jnp.where(lane == place_of(pair, pairs), value, norms[part])

    def place(p, top, bottom):
        top_sum, bottom_sum = square_sum(top), square_sum(bottom)
        if p == 0:
            put_split(moved_ref, 0, top)
            put_split(moved_ref, 2, jnp.where(is_first, bottom, top))
            mark(0, 1, jnp.where(is_first[:, :LANES], bottom_sum, top_sum))
            return
        put_split(moved_ref, 2 * p - 1, bottom)
        mark(1, p - 1, bottom_sum)
        if p == last:
            put_split(moved_ref, 2 * p + 1, top)
        else:
            put_split(moved_ref, 2 * p + 2, top)
            mark(0, p + 1, top_sum)

    turned_pairs((full0, rest0), (full1, rest1), blocks_ref, first_ref, last_ref, place)
    for p in range(1, last):
        kept[place_of(p, pairs)] = cross_twice(moved_ref[2 * p], moved_ref[2 * p + 1])
    kept[0] = kept[1] = jnp.zeros((BLOCK, LANES), f32)
    for q in range(pairs // 2):
        rows = slice((q % 2) * BLOCK, (q % 2 + 1) * BLOCK)
        packed_ref[q // 2, rows, :] = jnp.where(lane < BLOCK, kept[2 * q], kept[2 * q + 1])
    put_norms(packed_ref, jnp.concatenate(norms, axis=0).T)


def final_kernel(flags_ref, full0, rest0, full1, rest1, blocks_ref, first_ref, last_ref, out_ref, held, sems):
    pairs = blocks_ref.shape[0] // 2
    last = pairs - 1
    is_first = flag(flags_ref, 2, blocks_ref.shape[2])

    def send(slot, value):
        held[slot] = value
        pltpu.make_async_copy(held.at[slot], out_ref.at[slot], sems.at[slot]).start()

    def place(p, top, bottom):
        if p == 0:
            send(0, top)
            send(2, jnp.where(is_first, bottom, top))
        else:
            send(2 * p - 1, bottom)
            send(2 * p + 1 if p == last else 2 * p + 2, top)

    turned_pairs((full0, rest0), (full1, rest1), blocks_ref, first_ref, last_ref, place)
    for slot in range(2 * pairs):
        pltpu.make_async_copy(held.at[slot], out_ref.at[slot], sems.at[slot]).wait()


def move(flags, outer, inner, blocks, edges, final):
    count, _, length = blocks.shape
    first, last = edges
    if final:
        out_shape = jax.ShapeDtypeStruct((count, BLOCK, length), f32)
    else:
        out_shape = [
            jax.ShapeDtypeStruct(blocks.shape, bf16),
            jax.ShapeDtypeStruct((2, ROWS, LANES), f32),
        ]
    return pl.pallas_call(
        final_kernel if final else move_kernel,
        grid=(1,),
        in_specs=[VMEM] * 6 + [block_of(*first), block_of(*last)],
        out_specs=pl.BlockSpec(memory_space=pl.ANY) if final else [VMEM, VMEM],
        out_shape=out_shape,
        scratch_shapes=[pltpu.VMEM((count, BLOCK, length), f32), pltpu.SemaphoreType.DMA((count,))] if final else [],
        cost_estimate=pl.CostEstimate(flops=2 * 10**9, bytes_accessed=10**7, transcendentals=0),
        compiler_params=pltpu.CompilerParams(vmem_limit_bytes=24 << 20),
        name="final" if final else "move",
    )(flags, *outer, *inner, blocks, first[0], last[0])


def edge_kernel(flags_ref, packed_ref, even_ref, odd_ref, top0, bottom0, top1, bottom1, edge_ref, mine_ref, other_ref, packed):
    odd, is_first, is_last = (flag(flags_ref, row, even_ref.shape[1]) for row in (1, 2, 3))
    lane = lane_index(BLOCK)

    def whole(ref):
        return ref[0, :BLOCK, :].astype(f32) + ref[0, BLOCK:, :].astype(f32)

    from_even, from_odd = even_ref[...], odd_ref[...]
    new_top = jnp.where(is_first, whole(top0), jnp.where(odd, from_even, from_odd))
    new_bottom = jnp.where(is_last, whole(bottom1), jnp.where(odd, from_odd, from_even))
    put_split(edge_ref, 0, new_top)
    put_split(edge_ref, 1, new_bottom)
    packed[...] = packed_ref[...]
    packed[0, :BLOCK, :] = jnp.where(
        lane < BLOCK, cross_twice(edge_ref[0], bottom0[0]), cross_twice(top1[0], edge_ref[1])
    )
    norms = jnp.where(lane == 0, square_sum(new_top), 0.0)
    norms = jnp.concatenate([norms, jnp.where(lane == 1, square_sum(new_bottom), 0.0)], axis=0).T
    row = 2 * BLOCK
    top_lanes = lane[:1] < BLOCK
    packed[0, row : row + 1, :] = jnp.where(top_lanes, norms[0:1], packed[0, row : row + 1, :])
    packed[0, row + 1 : row + 2, :] = jnp.where(top_lanes, packed[0, row + 1 : row + 2, :], norms[1:2])
    put_halves(flags_ref, packed, mine_ref, other_ref)


def join(flags, packed, even, odd, moved):
    count, _, length = moved.shape
    half = jax.ShapeDtypeStruct((ROWS, LANES), f32)
    return pl.pallas_call(
        edge_kernel,
        grid=(1,),
        in_specs=[VMEM] * 4 + [block_of(moved, slot) for slot in (0, 1, count - 2, count - 1)],
        out_specs=[VMEM, VMEM, VMEM],
        out_shape=[jax.ShapeDtypeStruct((2, LANES, length), bf16), half, half],
        scratch_shapes=[pltpu.VMEM((2, ROWS, LANES), f32)],
        cost_estimate=pl.CostEstimate(flops=10**7, bytes_accessed=10**6, transcendentals=0),
        compiler_params=pltpu.CompilerParams(vmem_limit_bytes=8 << 20),
        name="join",
    )(flags, packed, even, odd, moved, moved, moved, moved)


def last_kernel(where_ref, even_ref, odd_ref, own_ref, out_ref, sems):
    del own_ref
    even = where_ref[1] == 0
    for edge in range(2):
        block = edge * (out_ref.shape[0] - 1)
        take = where_ref[2 + edge] == 0
        use_odd = even if edge == 0 else jnp.logical_not(even)
        for source, chosen in ((odd_ref, use_odd), (even_ref, jnp.logical_not(use_odd))):
            copy = pltpu.make_async_copy(source, out_ref.at[block], sems.at[edge])

            @pl.when(jnp.logical_and(take, chosen))
            def _():
                copy.start()

    for edge in range(2):
        block = edge * (out_ref.shape[0] - 1)

        @pl.when(where_ref[2 + edge] == 0)
        def _():
            pltpu.make_async_copy(odd_ref, out_ref.at[block], sems.at[edge]).wait()


def close(where, even, odd, out):
    return pl.pallas_call(
        last_kernel,
        in_specs=[SMEM, VMEM, VMEM, pl.BlockSpec(memory_space=pl.ANY)],
        out_specs=pl.BlockSpec(memory_space=pl.ANY),
        out_shape=jax.ShapeDtypeStruct(out.shape, f32),
        scratch_shapes=[pltpu.SemaphoreType.DMA((2,))],
        input_output_aliases={3: 0},
        compiler_params=pltpu.CompilerParams(vmem_limit_bytes=8 << 20),
        name="close",
    )(where, even, odd, out)


def exchange(value, bit):
    count = lax.axis_size("row")
    return lax.ppermute(value, "row", [(source, source ^ bit) for source in range(count)])


def row_sum(mine, other):
    count = lax.axis_size("row")
    total = mine + exchange(other, 1)
    if count == 8:
        near, far, across = exchange(total, 2), exchange(total, 4), exchange(total, 6)
        total = (total + near) + (far + across)
    else:
        bit = 2
        while bit < count:
            total = total + exchange(total, bit)
            bit *= 2
    return total, exchange(total, 1)


def swap_edges(even, odd):
    count = lax.axis_size("col")

    def between(start):
        pairs = [(left, left + 1) for left in range(start, count - 1, 2)]
        return pairs + [(right, left) for left, right in pairs]

    odd = lax.ppermute(odd, "col", between(1))
    return lax.ppermute(even, "col", between(0)), odd


def local(columns, block_order):
    width, length = columns.shape
    count = width // BLOCK
    assert count == 16 and lax.axis_size("row") % 2 == 0
    position = lax.axis_index("col")
    where = jnp.stack(
        [
            lax.axis_index("row") % 2,
            position % 2,
            (position == 0).astype(jnp.int32),
            (position == lax.axis_size("col") - 1).astype(jnp.int32),
        ]
    ).astype(jnp.int32)
    order = block_order - position * count
    flags = jnp.broadcast_to(jnp.concatenate([where, where])[:, None], (8, length))
    blocks, mine, other = start(columns.reshape(count, BLOCK, length), order, flags)
    edges = ((blocks, 0), (blocks, count - 1))
    for step in range(STEPS):
        final = step == STEPS - 1
        mine, other = row_sum(mine, other)
        full, rest, even, odd = outer_turns(flags, mine, other, blocks, edges)
        inner = inner_turns(flags, mine, other, full, count // 2)
        even, odd = swap_edges(even, odd)
        if final:
            out = move(flags, (full, rest), inner, blocks, edges, True)
            return close(where, even, odd, out).reshape(width, length)
        blocks, packed = move(flags, (full, rest), inner, blocks, edges, False)
        edge, mine, other = join(flags, packed, even, odd, blocks)
        edges = ((edge, 0), (edge, 1))


def solution(mesh):
    placed = (P("col", "row"), P("col"))
    return jax.shard_map(local, mesh=mesh, in_specs=placed, out_specs=P("col", "row"), check_vma=False)
```

```python
import jax
import jax.numpy as jnp
from jax import lax
from jax.experimental import pallas as pl
from jax.experimental.pallas import tpu as pltpu
from jax.sharding import PartitionSpec as P

BLOCK = 64
STEPS = 4
RANK = 8
LANES = 2 * BLOCK
AHEAD = 4
SENT = 5 * BLOCK // 2 + 8
ROWS = 2 * BLOCK + 8


f32 = jnp.float32
bf16 = jnp.bfloat16
SMEM = pl.BlockSpec(memory_space=pltpu.SMEM)
VMEM = pl.BlockSpec(memory_space=pltpu.VMEM)


def split(value):
    high = value.astype(bf16)
    low = (value - high.astype(f32)).astype(bf16)
    return high, low


def lane_index(rows):
    return lax.broadcasted_iota(jnp.int32, (rows, LANES), 1)


def put_split(ref, slot, value):
    high, low = split(value)
    ref[slot, :BLOCK, :] = high
    ref[slot, BLOCK:, :] = low


def cross_twice(top, bottom):
    gram = lax.dot_general(top, bottom, (((1,), (1,)), ((), ())), preferred_element_type=f32)
    folded = gram[:BLOCK] + gram[BLOCK:]
    return folded + pltpu.roll(folded, BLOCK, 1)


def square_sum(value):
    return jnp.sum(value * value, axis=1, keepdims=True)


def flag(flags_ref, row, lanes=LANES):
    return flags_ref[row : row + 1, :lanes] == 1


def put_halves(flags_ref, packed_ref, mine_ref, other_ref):
    core = flag(flags_ref, 0)
    half = BLOCK // 2
    norms = slice(2 * BLOCK, 2 * BLOCK + 4)
    first = (packed_ref[0, BLOCK : 2 * BLOCK, :], packed_ref[1, :half, :])
    second = (packed_ref[1, BLOCK : 2 * BLOCK, :], packed_ref[1, half:BLOCK, :])
    for ref, here, there in ((mine_ref, first, second), (other_ref, second, first)):
        ref[:BLOCK, :] = packed_ref[0, :BLOCK, :]
        ref[BLOCK : 2 * BLOCK, :] = jnp.where(core, there[0], here[0])
        ref[2 * BLOCK : 2 * BLOCK + half, :] = jnp.where(core, there[1], here[1])
        ref[2 * BLOCK + half :, :] = jnp.concatenate([packed_ref[0, norms, :], packed_ref[1, norms, :]], axis=0)


def place_of(pair, pairs):
    return 0 if pair == 0 else 1 if pair == pairs - 1 else pair + 1


def put_norms(packed_ref, by_place):
    for half in range(2):
        packed_ref[half, 2 * BLOCK : 2 * BLOCK + 4, :] = by_place[4 * half : 4 * half + 4]
        packed_ref[half, 2 * BLOCK + 4 :, :] = jnp.zeros((4, LANES), f32)


def start_kernel(order_ref, flags_ref, columns_ref, split_ref, mine_ref, other_ref, held, packed, sems):
    count = held.shape[0]
    pairs = count // 2
    lane = lane_index(BLOCK)

    def fetch(slot):
        return pltpu.make_async_copy(columns_ref.at[order_ref[slot]], held.at[slot], sems.at[slot])

    by_position = [0, pairs - 1] + list(range(1, pairs - 1))

    def ask(position):
        if position < pairs:
            fetch(2 * by_position[position]).start()
            fetch(2 * by_position[position] + 1).start()

    for position in range(AHEAD):
        ask(position)
    sums = [jnp.zeros((BLOCK, LANES), f32), jnp.zeros((BLOCK, LANES), f32)]
    crosses = []
    for position in range(pairs):
        pair = by_position[position]
        fetch(2 * pair).wait()
        fetch(2 * pair + 1).wait()
        ask(position + AHEAD)
        for half in range(2):
            slot = 2 * pair + half
            value = held[slot]
            put_split(split_ref, slot, value)
            sums[half] = jnp.where(lane == position, square_sum(value), sums[half])
        crosses.append(cross_twice(split_ref[2 * pair], split_ref[2 * pair + 1]))
    for q in range(pairs // 2):
        rows = slice((q % 2) * BLOCK, (q % 2 + 1) * BLOCK)
        packed[q // 2, rows, :] = jnp.where(lane < BLOCK, crosses[2 * q], crosses[2 * q + 1])
    put_norms(packed, jnp.concatenate(sums, axis=0).T)
    put_halves(flags_ref, packed, mine_ref, other_ref)


def start(columns, order, flags):
    count, _, length = columns.shape
    half = jax.ShapeDtypeStruct((SENT, LANES), f32)
    return pl.pallas_call(
        start_kernel,
        in_specs=[SMEM, VMEM, pl.BlockSpec(memory_space=pltpu.HBM)],
        out_specs=[VMEM, VMEM, VMEM],
        out_shape=[jax.ShapeDtypeStruct((count, LANES, length), bf16), half, half],
        scratch_shapes=[
            pltpu.VMEM((count, BLOCK, length), f32),
            pltpu.VMEM((2, ROWS, LANES), f32),
            pltpu.SemaphoreType.DMA((count,)),
        ],
        compiler_params=pltpu.CompilerParams(vmem_limit_bytes=46 << 20),
        name="start",
    )(order, flags, columns)


def row_of(value, index):
    return jnp.broadcast_to(value[index : index + 1, :], value.shape)


def eliminate(blocks, panels):
    size = len(blocks[0])
    sublane = lax.broadcasted_iota(jnp.int32, (size, LANES), 0)
    for j in range(size):
        here = sublane == j
        for q, work in enumerate(blocks):
            pivot_column = work[j]
            factor = jnp.where(here, pivot_column - 1.0, pivot_column) * (1.0 / row_of(pivot_column, j))

            def swept(value):
                return value - factor * row_of(value, j)

            for b in range(j + 1, size):
                work[b] = swept(work[b])
            panels[q] = swept(panels[q])
    return panels


def inverses(systems):
    lane = lane_index(RANK)
    base = (lane // BLOCK) * BLOCK
    eye = (lax.broadcasted_iota(jnp.int32, (RANK, LANES), 0) == lane % RANK).astype(f32)
    groups = BLOCK // RANK

    def sweep(r, work):
        pivots = (lane % BLOCK) // RANK == r
        columns = [[[None] * RANK for _ in range(groups)] for _ in work]
        for some in (range(1), range(1, groups)):
            for a in range(RANK):
                pick = base + (RANK * r + a)
                for g in some:
                    for q, rows in enumerate(work):
                        columns[q][g][a] = jnp.take_along_axis(rows[g], pick, axis=1, mode="promise_in_bounds")
        panels = eliminate(
            [list(columns[q][0]) for q in range(len(work))], [jnp.where(pivots, eye, rows[0]) for rows in work]
        )
        result = []
        for q, rows in enumerate(work):
            used = jnp.where(pivots, eye - panels[q], panels[q])
            update = [row_of(used, a) for a in range(RANK)]
            swept = []
            for g in range(1, groups):
                value = rows[g]
                for a in range(RANK):
                    value = value - columns[q][g][a] * update[a]
                swept.append(value)
            result.append(tuple(swept) + (jnp.where(pivots, -panels[q], panels[q]),))
        return tuple(result)

    work = tuple(tuple(system[RANK * g : RANK * (g + 1)] for g in range(groups)) for system in systems)
    work = lax.fori_loop(0, groups, sweep, work)
    return [-jnp.concatenate(rows, axis=0) for rows in work]


def split3(value):
    high = value.astype(bf16)
    rest = value - high.astype(f32)
    middle = rest.astype(bf16)
    return high, middle, (rest - middle.astype(f32)).astype(bf16)


def product3(left, right, transposed=False):
    axis = 1 if transposed else 0
    contract = (((1,), (axis,)), ((), ()))

    def dot(lefts, rights):
        return lax.dot_general(
            jnp.concatenate(lefts, axis=1), jnp.concatenate(rights, axis=axis), contract, preferred_element_type=f32
        )

    high, middle, low = left
    other_high, other_middle, other_low = right
    return (
        dot((low, high), (other_high, other_low))
        + dot((high, middle), (other_middle, other_middle))
        + dot((high, middle), (other_high, other_high))
    )


def apply_turn(full, rest, top, bottom):
    both = jnp.concatenate([top, bottom], axis=0)
    highs = jnp.concatenate([top[:BLOCK], bottom[:BLOCK]] * 2, axis=0)
    return jnp.dot(full, both, preferred_element_type=f32) + jnp.dot(rest, highs, preferred_element_type=f32)


def inner_crosses(flags_ref, mine_ref, other_ref):
    core = flag(flags_ref, 0)
    mine, other = mine_ref[BLOCK:, :], other_ref[BLOCK:, :]
    first, second = jnp.where(core, other, mine), jnp.where(core, mine, other)
    rest = slice(BLOCK, BLOCK + BLOCK // 2)
    return [first[:BLOCK], jnp.concatenate([first[rest], second[rest]], axis=0), second[:BLOCK]]


def couple(crosses, norm_rows, begin, left):
    by_column = norm_rows.T
    flipped = pltpu.roll(norm_rows, BLOCK, 1)
    couplings = []
    for q, cross in enumerate(crosses, begin):
        n0, n1 = 2 * q, 2 * q + 1
        bottom = jnp.where(left[:1], flipped[n0 : n0 + 1], norm_rows[n1 : n1 + 1])
        top = jnp.where(left, by_column[:BLOCK, n0 : n0 + 1], by_column[:BLOCK, n1 : n1 + 1])
        spread = bottom - top
        square = spread * spread + 4.0 * cross * cross
        scale = (top + bottom) / BLOCK
        couplings.append(2.0 * cross * spread / (square + jnp.abs(spread) * jnp.sqrt(square) + scale * scale))
    return couplings


def put_turns(couplings, full_ref, rest_ref):
    each = range(len(couplings))
    lane = lane_index(BLOCK)
    left = lane < BLOCK
    unit = (lax.broadcasted_iota(jnp.int32, (BLOCK, LANES), 0) == lane % BLOCK).astype(f32)

    def diagonal(value):
        zero = jnp.zeros_like(value)
        return jnp.concatenate([jnp.where(left, value, zero), jnp.where(left, zero, value)], axis=0)

    def turn_over(value):
        return pltpu.roll(value, BLOCK, 1)

    parts = [split3(coupling) for coupling in couplings]
    spread_parts = [tuple(diagonal(part) for part in parts[q]) for q in each]
    systems = [unit + product3(parts[q], spread_parts[q], True) for q in each]
    flips = [split3(jnp.concatenate([coupling, coupling], axis=0).T) for coupling in couplings]

    solved = inverses(systems)

    products = [product3(split3(solved[q]), spread_parts[q]) for q in each]
    residuals = [unit - solved[q] - product3(split3(products[q]), spread_parts[q], True) for q in each]
    steps = [
        jnp.dot(residuals[q].astype(bf16), diagonal(solved[q].astype(bf16)), preferred_element_type=f32) for q in each
    ]
    solved = [solved[q] + steps[q] for q in each]
    products = [
        products[q] + jnp.dot(steps[q].astype(bf16), spread_parts[q][0], preferred_element_type=f32) for q in each
    ]
    corners = []
    for q in each:
        high, middle, low = split3(products[q])
        flip_high, flip_middle, flip_low = flips[q]
        mixed = jnp.where(lane_index(LANES) < BLOCK, flip_low, flip_high)
        corners.append(
            jnp.dot(mixed, jnp.concatenate([high, low], axis=0), preferred_element_type=f32)
            + jnp.dot(
                jnp.concatenate([flip_high, flip_middle], axis=1),
                jnp.concatenate([high, middle, high, middle], axis=0),
                preferred_element_type=f32,
            )
        )
    products_t = [jnp.concatenate([product, product], axis=0).T for product in products]

    def put(pair, rows, top_part, bottom_part):
        full_ref[pair, rows, :LANES] = top_part.astype(bf16)
        full_ref[pair, rows, LANES:] = bottom_part.astype(bf16)
        _, middle, low = split3(jnp.where(left, top_part, bottom_part))
        rest_ref[pair, rows, :LANES] = middle
        rest_ref[pair, rows, LANES:] = low

    upper_rows, lower_rows = slice(0, BLOCK), slice(BLOCK, LANES)
    for q in each:
        pair = 2 * q
        inverse, product, corner = solved[q], products[q], corners[q]
        inverse_r, product_r = turn_over(inverse), turn_over(product)
        first_corner, second_corner = corner[:BLOCK], corner[BLOCK:]
        first_r, second_r = turn_over(first_corner), turn_over(second_corner)
        doubles = (
            (jnp.where(left, inverse, inverse_r), jnp.where(left, product, product_r), products_t[q][:BLOCK], jnp.where(left, first_corner, first_r)),
            (jnp.where(left, inverse_r, inverse), jnp.where(left, product_r, product), products_t[q][BLOCK:], jnp.where(left, second_r, second_corner)),
        )
        for h, (inverse2, product2, product_t2, corner2) in enumerate(doubles):
            put(pair + h, upper_rows, 2.0 * inverse2 - unit, -2.0 * product2)
            put(pair + h, lower_rows, 2.0 * product_t2, unit - 2.0 * corner2)


def outer_kernel(flags_ref, mine_ref, first_top, first_bottom, last_top, last_bottom, full_ref, rest_ref, even_ref, odd_ref):
    left = lane_index(BLOCK) < BLOCK
    put_turns(couple([mine_ref[:BLOCK, :]], mine_ref[SENT - 8 :, :], 0, left), full_ref, rest_ref)
    last_out = apply_turn(full_ref[1, :BLOCK, :], rest_ref[1, :BLOCK, :], last_top[0], last_bottom[0])
    first_out = apply_turn(full_ref[0, BLOCK:, :], rest_ref[0, BLOCK:, :], first_top[0], first_bottom[0])
    odd = flag(flags_ref, 1, last_out.shape[1])
    even_ref[...] = jnp.where(odd, first_out, last_out)
    odd_ref[...] = jnp.where(odd, last_out, first_out)


def inner_kernel(flags_ref, mine_ref, other_ref, after_ref, full_ref, rest_ref):
    del after_ref
    left = lane_index(BLOCK) < BLOCK
    crosses = inner_crosses(flags_ref, mine_ref, other_ref)
    put_turns(couple(crosses, mine_ref[SENT - 8 :, :], 1, left), full_ref, rest_ref)


def block_of(array, slot):
    return pl.BlockSpec((1,) + array.shape[1:], lambda *_: (slot, 0, 0))


def turn_shapes(pairs):
    return [jax.ShapeDtypeStruct((pairs, LANES, 2 * LANES), bf16)] * 2


def outer_turns(flags, mine, blocks, edges):
    count, _, length = blocks.shape
    first, last = edges
    sent = jax.ShapeDtypeStruct((BLOCK, length), f32)
    return pl.pallas_call(
        outer_kernel,
        grid=(1,),
        in_specs=[VMEM, VMEM, block_of(*first), block_of(blocks, 1), block_of(blocks, count - 2), block_of(*last)],
        out_specs=[VMEM] * 4,
        out_shape=turn_shapes(2) + [sent, sent],
        compiler_params=pltpu.CompilerParams(vmem_limit_bytes=12 << 20),
        cost_estimate=pl.CostEstimate(flops=10**7, bytes_accessed=10**6, transcendentals=0),
        name="outer",
    )(flags, mine, first[0], blocks, blocks, last[0])


def inner_turns(flags, mine, other, after, pairs):
    return pl.pallas_call(
        inner_kernel,
        in_specs=[VMEM, VMEM, VMEM, pl.BlockSpec(memory_space=pl.ANY)],
        out_specs=[VMEM] * 2,
        out_shape=turn_shapes(pairs - 2),
        compiler_params=pltpu.CompilerParams(vmem_limit_bytes=12 << 20),
        cost_estimate=pl.CostEstimate(flops=10**10, bytes_accessed=10**6, transcendentals=0),
        name="inner",
    )(flags, mine, other, after)


def turned_pairs(outer_refs, inner_refs, blocks_ref, first_ref, last_ref, place):
    pairs = blocks_ref.shape[0] // 2
    for p in range(pairs):
        top = first_ref[0] if p == 0 else blocks_ref[2 * p]
        bottom = last_ref[0] if p == pairs - 1 else blocks_ref[2 * p + 1]
        if p in (0, pairs - 1):
            full, rest = (ref[min(p, 1)] for ref in outer_refs)
        else:
            full, rest = (ref[p - 1] for ref in inner_refs)
        out = apply_turn(full, rest, top, bottom)
        place(p, out[:BLOCK], out[BLOCK:])


def move_kernel(flags_ref, full0, rest0, full1, rest1, blocks_ref, first_ref, last_ref, moved_ref, packed_ref):
    pairs = blocks_ref.shape[0] // 2
    last = pairs - 1
    is_first = flag(flags_ref, 2, blocks_ref.shape[2])
    lane = lane_index(BLOCK)
    norms = [jnp.zeros((BLOCK, LANES), f32), jnp.zeros((BLOCK, LANES), f32)]
    kept = {}

    def mark(part, pair, value):
        norms[part] = jnp.where(lane == place_of(pair, pairs), value, norms[part])

    def place(p, top, bottom):
        top_sum, bottom_sum = square_sum(top), square_sum(bottom)
        if p == 0:
            put_split(moved_ref, 0, top)
            put_split(moved_ref, 2, jnp.where(is_first, bottom, top))
            mark(0, 1, jnp.where(is_first[:, :LANES], bottom_sum, top_sum))
            return
        put_split(moved_ref, 2 * p - 1, bottom)
        mark(1, p - 1, bottom_sum)
        if p == last:
            put_split(moved_ref, 2 * p + 1, top)
        else:
            put_split(moved_ref, 2 * p + 2, top)
            mark(0, p + 1, top_sum)

    turned_pairs((full0, rest0), (full1, rest1), blocks_ref, first_ref, last_ref, place)
    for p in range(1, last):
        kept[place_of(p, pairs)] = cross_twice(moved_ref[2 * p], moved_ref[2 * p + 1])
    kept[0] = kept[1] = jnp.zeros((BLOCK, LANES), f32)
    for q in range(pairs // 2):
        rows = slice((q % 2) * BLOCK, (q % 2 + 1) * BLOCK)
        packed_ref[q // 2, rows, :] = jnp.where(lane < BLOCK, kept[2 * q], kept[2 * q + 1])
    put_norms(packed_ref, jnp.concatenate(norms, axis=0).T)


def final_kernel(flags_ref, full0, rest0, full1, rest1, blocks_ref, first_ref, last_ref, out_ref, held, sems):
    pairs = blocks_ref.shape[0] // 2
    last = pairs - 1
    is_first = flag(flags_ref, 2, blocks_ref.shape[2])

    def send(slot, value):
        held[slot] = value
        pltpu.make_async_copy(held.at[slot], out_ref.at[slot], sems.at[slot]).start()

    def place(p, top, bottom):
        if p == 0:
            send(0, top)
            send(2, jnp.where(is_first, bottom, top))
        else:
            send(2 * p - 1, bottom)
            send(2 * p + 1 if p == last else 2 * p + 2, top)

    turned_pairs((full0, rest0), (full1, rest1), blocks_ref, first_ref, last_ref, place)
    for slot in range(2 * pairs):
        pltpu.make_async_copy(held.at[slot], out_ref.at[slot], sems.at[slot]).wait()


def move(flags, outer, inner, blocks, edges, final):
    count, _, length = blocks.shape
    first, last = edges
    if final:
        out_shape = jax.ShapeDtypeStruct((count, BLOCK, length), f32)
    else:
        out_shape = [
            jax.ShapeDtypeStruct(blocks.shape, bf16),
            jax.ShapeDtypeStruct((2, ROWS, LANES), f32),
        ]
    return pl.pallas_call(
        final_kernel if final else move_kernel,
        grid=(1,),
        in_specs=[VMEM] * 6 + [block_of(*first), block_of(*last)],
        out_specs=pl.BlockSpec(memory_space=pl.ANY) if final else [VMEM, VMEM],
        out_shape=out_shape,
        scratch_shapes=[pltpu.VMEM((count, BLOCK, length), f32), pltpu.SemaphoreType.DMA((count,))] if final else [],
        cost_estimate=pl.CostEstimate(flops=2 * 10**9, bytes_accessed=10**7, transcendentals=0),
        compiler_params=pltpu.CompilerParams(vmem_limit_bytes=24 << 20),
        name="final" if final else "move",
    )(flags, *outer, *inner, blocks, first[0], last[0])


def edge_kernel(flags_ref, packed_ref, even_ref, odd_ref, top0, bottom0, top1, bottom1, edge_ref, mine_ref, other_ref, packed):
    odd, is_first, is_last = (flag(flags_ref, row, even_ref.shape[1]) for row in (1, 2, 3))
    lane = lane_index(BLOCK)

    def whole(ref):
        return ref[0, :BLOCK, :].astype(f32) + ref[0, BLOCK:, :].astype(f32)

    from_even, from_odd = even_ref[...], odd_ref[...]
    new_top = jnp.where(is_first, whole(top0), jnp.where(odd, from_even, from_odd))
    new_bottom = jnp.where(is_last, whole(bottom1), jnp.where(odd, from_odd, from_even))
    put_split(edge_ref, 0, new_top)
    put_split(edge_ref, 1, new_bottom)
    packed[...] = packed_ref[...]
    packed[0, :BLOCK, :] = jnp.where(
        lane < BLOCK, cross_twice(edge_ref[0], bottom0[0]), cross_twice(top1[0], edge_ref[1])
    )
    norms = jnp.where(lane == 0, square_sum(new_top), 0.0)
    norms = jnp.concatenate([norms, jnp.where(lane == 1, square_sum(new_bottom), 0.0)], axis=0).T
    row = 2 * BLOCK
    top_lanes = lane[:1] < BLOCK
    packed[0, row : row + 1, :] = jnp.where(top_lanes, norms[0:1], packed[0, row : row + 1, :])
    packed[0, row + 1 : row + 2, :] = jnp.where(top_lanes, packed[0, row + 1 : row + 2, :], norms[1:2])
    put_halves(flags_ref, packed, mine_ref, other_ref)


def join(flags, packed, even, odd, moved):
    count, _, length = moved.shape
    half = jax.ShapeDtypeStruct((SENT, LANES), f32)
    return pl.pallas_call(
        edge_kernel,
        grid=(1,),
        in_specs=[VMEM] * 4 + [block_of(moved, slot) for slot in (0, 1, count - 2, count - 1)],
        out_specs=[VMEM, VMEM, VMEM],
        out_shape=[jax.ShapeDtypeStruct((2, LANES, length), bf16), half, half],
        scratch_shapes=[pltpu.VMEM((2, ROWS, LANES), f32)],
        cost_estimate=pl.CostEstimate(flops=10**7, bytes_accessed=10**6, transcendentals=0),
        compiler_params=pltpu.CompilerParams(vmem_limit_bytes=8 << 20),
        name="join",
    )(flags, packed, even, odd, moved, moved, moved, moved)


def last_kernel(where_ref, even_ref, odd_ref, own_ref, out_ref, sems):
    del own_ref
    even = where_ref[1] == 0
    for edge in range(2):
        block = edge * (out_ref.shape[0] - 1)
        take = where_ref[2 + edge] == 0
        use_odd = even if edge == 0 else jnp.logical_not(even)
        for source, chosen in ((odd_ref, use_odd), (even_ref, jnp.logical_not(use_odd))):
            copy = pltpu.make_async_copy(source, out_ref.at[block], sems.at[edge])

            @pl.when(jnp.logical_and(take, chosen))
            def _():
                copy.start()

    for edge in range(2):
        block = edge * (out_ref.shape[0] - 1)

        @pl.when(where_ref[2 + edge] == 0)
        def _():
            pltpu.make_async_copy(odd_ref, out_ref.at[block], sems.at[edge]).wait()


def close(where, even, odd, out):
    return pl.pallas_call(
        last_kernel,
        in_specs=[SMEM, VMEM, VMEM, pl.BlockSpec(memory_space=pl.ANY)],
        out_specs=pl.BlockSpec(memory_space=pl.ANY),
        out_shape=jax.ShapeDtypeStruct(out.shape, f32),
        scratch_shapes=[pltpu.SemaphoreType.DMA((2,))],
        input_output_aliases={3: 0},
        compiler_params=pltpu.CompilerParams(vmem_limit_bytes=8 << 20),
        name="close",
    )(where, even, odd, out)


def exchange(value, bit):
    count = lax.axis_size("row")
    return lax.ppermute(value, "row", [(source, source ^ bit) for source in range(count)])


def row_sum(mine, other):
    count = lax.axis_size("row")
    total = mine + exchange(other, 1)
    if count == 8:
        near, far, across = exchange(total, 2), exchange(total, 4), exchange(total, 6)
        total = (total + near) + (far + across)
    else:
        bit = 2
        while bit < count:
            total = total + exchange(total, bit)
            bit *= 2
    return total, exchange(total, 1)


def swap_edges(even, odd):
    count = lax.axis_size("col")

    def between(start):
        pairs = [(left, left + 1) for left in range(start, count - 1, 2)]
        return pairs + [(right, left) for left, right in pairs]

    odd = lax.ppermute(odd, "col", between(1))
    return lax.ppermute(even, "col", between(0)), odd


def local(columns, block_order):
    width, length = columns.shape
    count = width // BLOCK
    assert count == 16 and lax.axis_size("row") % 2 == 0
    position = lax.axis_index("col")
    where = jnp.stack(
        [
            lax.axis_index("row") % 2,
            position % 2,
            (position == 0).astype(jnp.int32),
            (position == lax.axis_size("col") - 1).astype(jnp.int32),
        ]
    ).astype(jnp.int32)
    order = block_order - position * count
    flags = jnp.broadcast_to(jnp.concatenate([where, where])[:, None], (8, length))
    blocks, mine, other = start(columns.reshape(count, BLOCK, length), order, flags)
    edges = ((blocks, 0), (blocks, count - 1))
    for step in range(STEPS):
        final = step == STEPS - 1
        mine, other = row_sum(mine, other)
        full, rest, even, odd = outer_turns(flags, mine, blocks, edges)
        inner = inner_turns(flags, mine, other, full, count // 2)
        even, odd = swap_edges(even, odd)
        if final:
            out = move(flags, (full, rest), inner, blocks, edges, True)
            return close(where, even, odd, out).reshape(width, length)
        blocks, packed = move(flags, (full, rest), inner, blocks, edges, False)
        edge, mine, other = join(flags, packed, even, odd, blocks)
        edges = ((edge, 0), (edge, 1))


def solution(mesh):
    placed = (P("col", "row"), P("col"))
    return jax.shard_map(local, mesh=mesh, in_specs=placed, out_specs=P("col", "row"), check_vma=False)
```

```python
import jax
import jax.numpy as jnp
from jax import lax
from jax.experimental import pallas as pl
from jax.experimental.pallas import tpu as pltpu
from jax.sharding import PartitionSpec as P

BLOCK = 64
STEPS = 4
RANK = 8
LANES = 2 * BLOCK
AHEAD = 4
SENT = 5 * BLOCK // 2 + 8
ROWS = 2 * BLOCK + 8


f32 = jnp.float32
bf16 = jnp.bfloat16
SMEM = pl.BlockSpec(memory_space=pltpu.SMEM)
VMEM = pl.BlockSpec(memory_space=pltpu.VMEM)


def split(value):
    high = value.astype(bf16)
    low = (value - high.astype(f32)).astype(bf16)
    return high, low


def lane_index(rows):
    return lax.broadcasted_iota(jnp.int32, (rows, LANES), 1)


def put_split(ref, slot, value):
    high, low = split(value)
    ref[slot, :BLOCK, :] = high
    ref[slot, BLOCK:, :] = low


def cross_twice(top, bottom):
    gram = lax.dot_general(top, bottom, (((1,), (1,)), ((), ())), preferred_element_type=f32)
    folded = gram[:BLOCK] + gram[BLOCK:]
    return folded + pltpu.roll(folded, BLOCK, 1)


def square_sum(value):
    return jnp.sum(value * value, axis=1, keepdims=True)


def flag(flags_ref, row, lanes=LANES):
    return flags_ref[row : row + 1, :lanes] == 1


def put_halves(flags_ref, packed_ref, mine_ref, other_ref):
    core = flag(flags_ref, 0)
    half = BLOCK // 2
    norms = slice(2 * BLOCK, 2 * BLOCK + 4)
    first = (packed_ref[0, BLOCK : 2 * BLOCK, :], packed_ref[1, :half, :])
    second = (packed_ref[1, BLOCK : 2 * BLOCK, :], packed_ref[1, half:BLOCK, :])
    for ref, here, there in ((mine_ref, first, second), (other_ref, second, first)):
        ref[:BLOCK, :] = packed_ref[0, :BLOCK, :]
        ref[BLOCK : 2 * BLOCK, :] = jnp.where(core, there[0], here[0])
        ref[2 * BLOCK : 2 * BLOCK + half, :] = jnp.where(core, there[1], here[1])
        ref[2 * BLOCK + half :, :] = jnp.concatenate([packed_ref[0, norms, :], packed_ref[1, norms, :]], axis=0)


def place_of(pair, pairs):
    return 0 if pair == 0 else 1 if pair == pairs - 1 else pair + 1


def put_norms(packed_ref, by_place):
    for half in range(2):
        packed_ref[half, 2 * BLOCK : 2 * BLOCK + 4, :] = by_place[4 * half : 4 * half + 4]
        packed_ref[half, 2 * BLOCK + 4 :, :] = jnp.zeros((4, LANES), f32)


def start_kernel(order_ref, flags_ref, columns_ref, split_ref, mine_ref, other_ref, held, packed, sems):
    count = held.shape[0]
    pairs = count // 2
    lane = lane_index(BLOCK)

    def fetch(slot):
        return pltpu.make_async_copy(columns_ref.at[order_ref[slot]], held.at[slot], sems.at[slot])

    by_position = [0, pairs - 1] + list(range(1, pairs - 1))

    def ask(position):
        if position < pairs:
            fetch(2 * by_position[position]).start()
            fetch(2 * by_position[position] + 1).start()

    for position in range(AHEAD):
        ask(position)
    sums = [jnp.zeros((BLOCK, LANES), f32), jnp.zeros((BLOCK, LANES), f32)]
    crosses = []
    for position in range(pairs):
        pair = by_position[position]
        fetch(2 * pair).wait()
        fetch(2 * pair + 1).wait()
        ask(position + AHEAD)
        for half in range(2):
            slot = 2 * pair + half
            value = held[slot]
            put_split(split_ref, slot, value)
            sums[half] = jnp.where(lane == position, square_sum(value), sums[half])
        crosses.append(cross_twice(split_ref[2 * pair], split_ref[2 * pair + 1]))
    for q in range(pairs // 2):
        rows = slice((q % 2) * BLOCK, (q % 2 + 1) * BLOCK)
        packed[q // 2, rows, :] = jnp.where(lane < BLOCK, crosses[2 * q], crosses[2 * q + 1])
    put_norms(packed, jnp.concatenate(sums, axis=0).T)
    put_halves(flags_ref, packed, mine_ref, other_ref)


def start(columns, order, flags):
    count, _, length = columns.shape
    half = jax.ShapeDtypeStruct((SENT, LANES), f32)
    return pl.pallas_call(
        start_kernel,
        in_specs=[SMEM, VMEM, pl.BlockSpec(memory_space=pltpu.HBM)],
        out_specs=[VMEM, VMEM, VMEM],
        out_shape=[jax.ShapeDtypeStruct((count, LANES, length), bf16), half, half],
        scratch_shapes=[
            pltpu.VMEM((count, BLOCK, length), f32),
            pltpu.VMEM((2, ROWS, LANES), f32),
            pltpu.SemaphoreType.DMA((count,)),
        ],
        compiler_params=pltpu.CompilerParams(vmem_limit_bytes=46 << 20),
        name="start",
    )(order, flags, columns)


def row_of(value, index):
    return jnp.broadcast_to(value[index : index + 1, :], value.shape)


def eliminate(blocks, panels):
    size = len(blocks[0])
    sublane = lax.broadcasted_iota(jnp.int32, (size, LANES), 0)
    for j in range(size):
        here = sublane == j
        for q, work in enumerate(blocks):
            pivot_column = work[j]
            factor = jnp.where(here, pivot_column - 1.0, pivot_column) * (1.0 / row_of(pivot_column, j))

            def swept(value):
                return value - factor * row_of(value, j)

            for b in range(j + 1, size):
                work[b] = swept(work[b])
            panels[q] = swept(panels[q])
    return panels


def inverses(systems):
    lane = lane_index(RANK)
    base = (lane // BLOCK) * BLOCK
    eye = (lax.broadcasted_iota(jnp.int32, (RANK, LANES), 0) == lane % RANK).astype(f32)
    groups = BLOCK // RANK

    def sweep(r, work):
        pivots = (lane % BLOCK) // RANK == r
        columns = [[[None] * RANK for _ in range(groups)] for _ in work]
        for some in (range(1), range(1, groups)):
            for a in range(RANK):
                pick = base + (RANK * r + a)
                for g in some:
                    for q, rows in enumerate(work):
                        columns[q][g][a] = jnp.take_along_axis(rows[g], pick, axis=1, mode="promise_in_bounds")
        panels = eliminate(
            [list(columns[q][0]) for q in range(len(work))], [jnp.where(pivots, eye, rows[0]) for rows in work]
        )
        result = []
        for q, rows in enumerate(work):
            used = jnp.where(pivots, eye - panels[q], panels[q])
            update = [row_of(used, a) for a in range(RANK)]
            swept = []
            for g in range(1, groups):
                value = rows[g]
                for a in range(RANK):
                    value = value - columns[q][g][a] * update[a]
                swept.append(value)
            result.append(tuple(swept) + (jnp.where(pivots, -panels[q], panels[q]),))
        return tuple(result)

    work = tuple(tuple(system[RANK * g : RANK * (g + 1)] for g in range(groups)) for system in systems)
    work = lax.fori_loop(0, groups, sweep, work)
    return [-jnp.concatenate(rows, axis=0) for rows in work]


def split3(value):
    high = value.astype(bf16)
    rest = value - high.astype(f32)
    middle = rest.astype(bf16)
    return high, middle, (rest - middle.astype(f32)).astype(bf16)


def product3(left, right, transposed=False):
    axis = 1 if transposed else 0
    contract = (((1,), (axis,)), ((), ()))

    def dot(lefts, rights):
        return lax.dot_general(
            jnp.concatenate(lefts, axis=1), jnp.concatenate(rights, axis=axis), contract, preferred_element_type=f32
        )

    high, middle, low = left
    other_high, other_middle, other_low = right
    return (
        dot((low, high), (other_high, other_low))
        + dot((high, middle), (other_middle, other_middle))
        + dot((high, middle), (other_high, other_high))
    )


def apply_turn(full, rest, top, bottom):
    both = jnp.concatenate([top, bottom], axis=0)
    highs = jnp.concatenate([top[:BLOCK], bottom[:BLOCK]] * 2, axis=0)
    return jnp.dot(full, both, preferred_element_type=f32) + jnp.dot(rest, highs, preferred_element_type=f32)


def inner_crosses(flags_ref, mine_ref, other_ref):
    core = flag(flags_ref, 0)
    mine, other = mine_ref[BLOCK:, :], other_ref[BLOCK:, :]
    first, second = jnp.where(core, other, mine), jnp.where(core, mine, other)
    rest = slice(BLOCK, BLOCK + BLOCK // 2)
    return [first[:BLOCK], jnp.concatenate([first[rest], second[rest]], axis=0), second[:BLOCK]]


def couple(crosses, norm_rows, begin, left):
    by_column = norm_rows.T
    flipped = pltpu.roll(norm_rows, BLOCK, 1)
    couplings = []
    for q, cross in enumerate(crosses, begin):
        n0, n1 = 2 * q, 2 * q + 1
        bottom = jnp.where(left[:1], flipped[n0 : n0 + 1], norm_rows[n1 : n1 + 1])
        top = jnp.where(left, by_column[:BLOCK, n0 : n0 + 1], by_column[:BLOCK, n1 : n1 + 1])
        spread = bottom - top
        square = spread * spread + 4.0 * cross * cross
        scale = (top + bottom) / BLOCK
        couplings.append(2.0 * cross * spread / (square + jnp.abs(spread) * jnp.sqrt(square) + scale * scale))
    return couplings


def put_turns(couplings, full_ref, rest_ref):
    each = range(len(couplings))
    lane = lane_index(BLOCK)
    left = lane < BLOCK
    unit = (lax.broadcasted_iota(jnp.int32, (BLOCK, LANES), 0) == lane % BLOCK).astype(f32)

    def diagonal(value):
        zero = jnp.zeros_like(value)
        return jnp.concatenate([jnp.where(left, value, zero), jnp.where(left, zero, value)], axis=0)

    def turn_over(value):
        return pltpu.roll(value, BLOCK, 1)

    parts = [split3(coupling) for coupling in couplings]
    spread_parts = [tuple(diagonal(part) for part in parts[q]) for q in each]
    systems = [unit + product3(parts[q], spread_parts[q], True) for q in each]
    flips = [split3(jnp.concatenate([coupling, coupling], axis=0).T) for coupling in couplings]

    solved = inverses(systems)

    products = [product3(split3(solved[q]), spread_parts[q]) for q in each]
    residuals = [unit - solved[q] - product3(split3(products[q]), spread_parts[q], True) for q in each]
    steps = [
        jnp.dot(residuals[q].astype(bf16), diagonal(solved[q].astype(bf16)), preferred_element_type=f32) for q in each
    ]
    solved = [solved[q] + steps[q] for q in each]
    products = [
        products[q] + jnp.dot(steps[q].astype(bf16), spread_parts[q][0], preferred_element_type=f32) for q in each
    ]
    corners = []
    for q in each:
        high, middle, low = split3(products[q])
        flip_high, flip_middle, flip_low = flips[q]
        mixed = jnp.where(lane_index(LANES) < BLOCK, flip_low, flip_high)
        corners.append(
            jnp.dot(mixed, jnp.concatenate([high, low], axis=0), preferred_element_type=f32)
            + jnp.dot(
                jnp.concatenate([flip_high, flip_middle], axis=1),
                jnp.concatenate([high, middle, high, middle], axis=0),
                preferred_element_type=f32,
            )
        )
    products_t = [jnp.concatenate([product, product], axis=0).T for product in products]

    def put(pair, rows, top_part, bottom_part):
        full_ref[pair, rows, :LANES] = top_part.astype(bf16)
        full_ref[pair, rows, LANES:] = bottom_part.astype(bf16)
        _, middle, low = split3(jnp.where(left, top_part, bottom_part))
        rest_ref[pair, rows, :LANES] = middle
        rest_ref[pair, rows, LANES:] = low

    upper_rows, lower_rows = slice(0, BLOCK), slice(BLOCK, LANES)
    for q in each:
        pair = 2 * q
        inverse, product, corner = solved[q], products[q], corners[q]
        inverse_r, product_r = turn_over(inverse), turn_over(product)
        first_corner, second_corner = corner[:BLOCK], corner[BLOCK:]
        first_r, second_r = turn_over(first_corner), turn_over(second_corner)
        doubles = (
            (jnp.where(left, inverse, inverse_r), jnp.where(left, product, product_r), products_t[q][:BLOCK], jnp.where(left, first_corner, first_r)),
            (jnp.where(left, inverse_r, inverse), jnp.where(left, product_r, product), products_t[q][BLOCK:], jnp.where(left, second_r, second_corner)),
        )
        for h, (inverse2, product2, product_t2, corner2) in enumerate(doubles):
            put(pair + h, upper_rows, 2.0 * inverse2 - unit, -2.0 * product2)
            put(pair + h, lower_rows, 2.0 * product_t2, unit - 2.0 * corner2)


def outer_kernel(flags_ref, mine_ref, first_top, first_bottom, last_top, last_bottom, full_ref, rest_ref, even_ref, odd_ref):
    left = lane_index(BLOCK) < BLOCK
    put_turns(couple([mine_ref[:BLOCK, :]], mine_ref[SENT - 8 :, :], 0, left), full_ref, rest_ref)
    last_out = apply_turn(full_ref[1, :BLOCK, :], rest_ref[1, :BLOCK, :], last_top[0], last_bottom[0])
    first_out = apply_turn(full_ref[0, BLOCK:, :], rest_ref[0, BLOCK:, :], first_top[0], first_bottom[0])
    odd = flag(flags_ref, 1, last_out.shape[1])
    even_ref[...] = jnp.where(odd, first_out, last_out)
    odd_ref[...] = jnp.where(odd, last_out, first_out)


def inner_kernel(flags_ref, mine_ref, other_ref, after_ref, full_ref, rest_ref):
    del after_ref
    left = lane_index(BLOCK) < BLOCK
    crosses = inner_crosses(flags_ref, mine_ref, other_ref)
    put_turns(couple(crosses, mine_ref[SENT - 8 :, :], 1, left), full_ref, rest_ref)


def block_of(array, slot):
    return pl.BlockSpec((1,) + array.shape[1:], lambda *_: (slot, 0, 0))


def turn_shapes(pairs):
    return [jax.ShapeDtypeStruct((pairs, LANES, 2 * LANES), bf16)] * 2


def outer_turns(flags, mine, blocks, edges):
    count, _, length = blocks.shape
    first, last = edges
    sent = jax.ShapeDtypeStruct((BLOCK, length), f32)
    return pl.pallas_call(
        outer_kernel,
        grid=(1,),
        in_specs=[VMEM, VMEM, block_of(*first), block_of(blocks, 1), block_of(blocks, count - 2), block_of(*last)],
        out_specs=[VMEM] * 4,
        out_shape=turn_shapes(2) + [sent, sent],
        compiler_params=pltpu.CompilerParams(vmem_limit_bytes=12 << 20),
        cost_estimate=pl.CostEstimate(flops=10**7, bytes_accessed=10**6, transcendentals=0),
        name="outer",
    )(flags, mine, first[0], blocks, blocks, last[0])


def inner_turns(flags, mine, other, after, pairs):
    return pl.pallas_call(
        inner_kernel,
        in_specs=[VMEM, VMEM, VMEM, pl.BlockSpec(memory_space=pl.ANY)],
        out_specs=[VMEM] * 2,
        out_shape=turn_shapes(pairs - 2),
        compiler_params=pltpu.CompilerParams(vmem_limit_bytes=12 << 20),
        cost_estimate=pl.CostEstimate(flops=10**10, bytes_accessed=10**6, transcendentals=0),
        name="inner",
    )(flags, mine, other, after)


def turned_pairs(outer_refs, inner_refs, blocks_ref, first_ref, last_ref, place):
    pairs = blocks_ref.shape[0] // 2
    for p in range(pairs):
        top = first_ref[0] if p == 0 else blocks_ref[2 * p]
        bottom = last_ref[0] if p == pairs - 1 else blocks_ref[2 * p + 1]
        if p in (0, pairs - 1):
            full, rest = (ref[min(p, 1)] for ref in outer_refs)
        else:
            full, rest = (ref[p - 1] for ref in inner_refs)
        out = apply_turn(full, rest, top, bottom)
        place(p, out[:BLOCK], out[BLOCK:])


def move_kernel(flags_ref, full0, rest0, full1, rest1, blocks_ref, first_ref, last_ref, moved_ref, packed_ref):
    pairs = blocks_ref.shape[0] // 2
    last = pairs - 1
    is_first = flag(flags_ref, 2, blocks_ref.shape[2])
    lane = lane_index(BLOCK)
    norms = [jnp.zeros((BLOCK, LANES), f32), jnp.zeros((BLOCK, LANES), f32)]
    kept = {}

    def mark(part, pair, value):
        norms[part] = jnp.where(lane == place_of(pair, pairs), value, norms[part])

    def place(p, top, bottom):
        top_sum, bottom_sum = square_sum(top), square_sum(bottom)
        if p == 0:
            put_split(moved_ref, 0, top)
            put_split(moved_ref, 2, jnp.where(is_first, bottom, top))
            mark(0, 1, jnp.where(is_first[:, :LANES], bottom_sum, top_sum))
            return
        put_split(moved_ref, 2 * p - 1, bottom)
        mark(1, p - 1, bottom_sum)
        if p == last:
            put_split(moved_ref, 2 * p + 1, top)
        else:
            put_split(moved_ref, 2 * p + 2, top)
            mark(0, p + 1, top_sum)

    turned_pairs((full0, rest0), (full1, rest1), blocks_ref, first_ref, last_ref, place)
    for p in range(1, last):
        kept[place_of(p, pairs)] = cross_twice(moved_ref[2 * p], moved_ref[2 * p + 1])
    kept[0] = kept[1] = jnp.zeros((BLOCK, LANES), f32)
    for q in range(pairs // 2):
        rows = slice((q % 2) * BLOCK, (q % 2 + 1) * BLOCK)
        packed_ref[q // 2, rows, :] = jnp.where(lane < BLOCK, kept[2 * q], kept[2 * q + 1])
    put_norms(packed_ref, jnp.concatenate(norms, axis=0).T)


def final_kernel(flags_ref, full0, rest0, full1, rest1, blocks_ref, first_ref, last_ref, out_ref, held, sems):
    pairs = blocks_ref.shape[0] // 2
    last = pairs - 1
    is_first = flag(flags_ref, 2, blocks_ref.shape[2])

    def send(slot, value):
        held[slot] = value
        pltpu.make_async_copy(held.at[slot], out_ref.at[slot], sems.at[slot]).start()

    def place(p, top, bottom):
        if p == 0:
            send(0, top)
            send(2, jnp.where(is_first, bottom, top))
        else:
            send(2 * p - 1, bottom)
            send(2 * p + 1 if p == last else 2 * p + 2, top)

    turned_pairs((full0, rest0), (full1, rest1), blocks_ref, first_ref, last_ref, place)
    for slot in range(2 * pairs):
        pltpu.make_async_copy(held.at[slot], out_ref.at[slot], sems.at[slot]).wait()


def move(flags, outer, inner, blocks, edges, final):
    count, _, length = blocks.shape
    first, last = edges
    if final:
        out_shape = jax.ShapeDtypeStruct((count, BLOCK, length), f32)
    else:
        out_shape = [
            jax.ShapeDtypeStruct(blocks.shape, bf16),
            jax.ShapeDtypeStruct((2, ROWS, LANES), f32),
        ]
    return pl.pallas_call(
        final_kernel if final else move_kernel,
        grid=(1,),
        in_specs=[VMEM] * 6 + [block_of(*first), block_of(*last)],
        out_specs=pl.BlockSpec(memory_space=pl.ANY) if final else [VMEM, VMEM],
        out_shape=out_shape,
        scratch_shapes=[pltpu.VMEM((count, BLOCK, length), f32), pltpu.SemaphoreType.DMA((count,))] if final else [],
        cost_estimate=pl.CostEstimate(flops=2 * 10**9, bytes_accessed=10**7, transcendentals=0),
        compiler_params=pltpu.CompilerParams(vmem_limit_bytes=24 << 20),
        name="final" if final else "move",
    )(flags, *outer, *inner, blocks, first[0], last[0])


def edge_kernel(flags_ref, packed_ref, even_ref, odd_ref, top0, bottom0, top1, bottom1, edge_ref, mine_ref, other_ref, packed):
    odd, is_first, is_last = (flag(flags_ref, row, even_ref.shape[1]) for row in (1, 2, 3))
    lane = lane_index(BLOCK)

    def whole(ref):
        return ref[0, :BLOCK, :].astype(f32) + ref[0, BLOCK:, :].astype(f32)

    from_even, from_odd = even_ref[...], odd_ref[...]
    new_top = jnp.where(is_first, whole(top0), jnp.where(odd, from_even, from_odd))
    new_bottom = jnp.where(is_last, whole(bottom1), jnp.where(odd, from_odd, from_even))
    put_split(edge_ref, 0, new_top)
    put_split(edge_ref, 1, new_bottom)
    packed[...] = packed_ref[...]
    packed[0, :BLOCK, :] = jnp.where(
        lane < BLOCK, cross_twice(edge_ref[0], bottom0[0]), cross_twice(top1[0], edge_ref[1])
    )
    norms = jnp.where(lane == 0, square_sum(new_top), 0.0)
    norms = jnp.concatenate([norms, jnp.where(lane == 1, square_sum(new_bottom), 0.0)], axis=0).T
    row = 2 * BLOCK
    top_lanes = lane[:1] < BLOCK
    packed[0, row : row + 1, :] = jnp.where(top_lanes, norms[0:1], packed[0, row : row + 1, :])
    packed[0, row + 1 : row + 2, :] = jnp.where(top_lanes, packed[0, row + 1 : row + 2, :], norms[1:2])
    put_halves(flags_ref, packed, mine_ref, other_ref)


def join(flags, packed, even, odd, moved):
    count, _, length = moved.shape
    half = jax.ShapeDtypeStruct((SENT, LANES), f32)
    return pl.pallas_call(
        edge_kernel,
        grid=(1,),
        in_specs=[VMEM] * 4 + [block_of(moved, slot) for slot in (0, 1, count - 2, count - 1)],
        out_specs=[VMEM, VMEM, VMEM],
        out_shape=[jax.ShapeDtypeStruct((2, LANES, length), bf16), half, half],
        scratch_shapes=[pltpu.VMEM((2, ROWS, LANES), f32)],
        cost_estimate=pl.CostEstimate(flops=10**7, bytes_accessed=10**6, transcendentals=0),
        compiler_params=pltpu.CompilerParams(vmem_limit_bytes=8 << 20),
        name="join",
    )(flags, packed, even, odd, moved, moved, moved, moved)


def last_kernel(flags_ref, even_ref, odd_ref, own_ref, out_ref, sems):
    del own_ref
    odd, is_first, is_last = (jnp.max(flags_ref[row : row + 1, :LANES].astype(f32)) > 0.5 for row in (1, 2, 3))
    even = jnp.logical_not(odd)
    takes = (jnp.logical_not(is_first), jnp.logical_not(is_last))
    for edge in range(2):
        block = edge * (out_ref.shape[0] - 1)
        take = takes[edge]
        use_odd = even if edge == 0 else odd
        for source, chosen in ((odd_ref, use_odd), (even_ref, jnp.logical_not(use_odd))):
            copy = pltpu.make_async_copy(source, out_ref.at[block], sems.at[edge])

            @pl.when(jnp.logical_and(take, chosen))
            def _():
                copy.start()

    for edge in range(2):
        block = edge * (out_ref.shape[0] - 1)

        @pl.when(takes[edge])
        def _():
            pltpu.make_async_copy(odd_ref, out_ref.at[block], sems.at[edge]).wait()


def close(flags, even, odd, out):
    return pl.pallas_call(
        last_kernel,
        in_specs=[VMEM, VMEM, VMEM, pl.BlockSpec(memory_space=pl.ANY)],
        out_specs=pl.BlockSpec(memory_space=pl.ANY),
        out_shape=jax.ShapeDtypeStruct(out.shape, f32),
        scratch_shapes=[pltpu.SemaphoreType.DMA((2,))],
        input_output_aliases={3: 0},
        compiler_params=pltpu.CompilerParams(vmem_limit_bytes=8 << 20),
        name="close",
    )(flags, even, odd, out)


def exchange(value, bit):
    count = lax.axis_size("row")
    return lax.ppermute(value, "row", [(source, source ^ bit) for source in range(count)])


def row_sum(mine, other):
    count = lax.axis_size("row")
    total = mine + exchange(other, 1)
    if count == 8:
        near, far, across = exchange(total, 2), exchange(total, 4), exchange(total, 6)
        total = (total + near) + (far + across)
    else:
        bit = 2
        while bit < count:
            total = total + exchange(total, bit)
            bit *= 2
    return total, exchange(total, 1)


def swap_edges(even, odd):
    count = lax.axis_size("col")

    def between(start):
        pairs = [(left, left + 1) for left in range(start, count - 1, 2)]
        return pairs + [(right, left) for left, right in pairs]

    odd = lax.ppermute(odd, "col", between(1))
    return lax.ppermute(even, "col", between(0)), odd


def local(columns, block_order):
    width, length = columns.shape
    count = width // BLOCK
    assert count == 16 and lax.axis_size("row") % 2 == 0
    position = lax.axis_index("col")
    where = jnp.stack(
        [
            lax.axis_index("row") % 2,
            position % 2,
            (position == 0).astype(jnp.int32),
            (position == lax.axis_size("col") - 1).astype(jnp.int32),
        ]
    ).astype(jnp.int32)
    order = block_order - position * count
    flags = jnp.broadcast_to(jnp.concatenate([where, where])[:, None], (8, length))
    blocks, mine, other = start(columns.reshape(count, BLOCK, length), order, flags)
    edges = ((blocks, 0), (blocks, count - 1))
    for step in range(STEPS):
        final = step == STEPS - 1
        mine, other = row_sum(mine, other)
        full, rest, even, odd = outer_turns(flags, mine, blocks, edges)
        inner = inner_turns(flags, mine, other, full, count // 2)
        even, odd = swap_edges(even, odd)
        if final:
            out = move(flags, (full, rest), inner, blocks, edges, True)
            return close(flags, even, odd, out).reshape(width, length)
        blocks, packed = move(flags, (full, rest), inner, blocks, edges, False)
        edge, mine, other = join(flags, packed, even, odd, blocks)
        edges = ((edge, 0), (edge, 1))


def solution(mesh):
    placed = (P("col", "row"), P("col"))
    return jax.shard_map(local, mesh=mesh, in_specs=placed, out_specs=P("col", "row"), check_vma=False)
```
